128 devices in a mesh: gx: 2 (over core), gy: 64 (over z, y, x).
Axes of the slice: x: 4, y: 4, z: 4, core: 2. Of those that a mesh axis runs over, the one named last changes fastest.
Arguments:
- right_side: float32 [128, 16384], P('gx', 'gy'), may hold values from -34 to 34, as said below
- initial: float32 [128, 16384], P('gx', 'gy'), may hold values from -0.6 to 0.6
- reaction: float32 [128, 16384], P('gx', 'gy'), may hold values from 0.05 to 0.5
- velocity_x: float32 [128, 16384], P('gx', 'gy'), may hold values from -1 to 1
- velocity_y: float32 [128, 16384], P('gx', 'gy'), may hold values from -1 to 1
Outputs:
- solution: float32 [128, 16384], P('gx', 'gy')
- residual: float32 [128, 16384], P('gx', 'gy')
The draws below stay inside these ranges and needn't reach their ends.
Inputs may be any that keep to these rules, and one draw needn't show every extreme that they name: right_side is noise bounded by 4 in size times an envelope 0.5 + 8 g, where g is a periodic Gaussian bump of one device block's width along each dimension centred at a drawn position, so its entries lie within -34 and 34.
All inputs are finite; a program needn't handle non-finite values.
Results may differ from the reference program's by a relative error of at most 0.0075.
Values sent between devices are 32-bit elements.
No kernel may reach another device: no remote copies, remote signals or barrier semaphores. Data moves between devices by JAX's collectives and lax.ppermute only.
A program may use at most 64 MiB of HBM per device.

```python
import math
import jax
import jax.numpy as jnp
from jax import lax

CX = 64
CY = 256
RESTART = 15
NX = 128
NY = 16384


def draw_right_side(key, part):
    noise_key = jax.random.fold_in(key, 11)
    centre_key = jax.random.fold_in(key, 12)
    noise = jnp.clip(jax.random.normal(noise_key, (NX, NY), jnp.float32), -4.0, 4.0)
    centre = jax.random.uniform(centre_key, (2,), jnp.float32)
    along_x = jnp.mod(jnp.arange(NX, dtype=jnp.float32) - centre[0] * NX, NX)
    along_y = jnp.mod(jnp.arange(NY, dtype=jnp.float32) - centre[1] * NY, NY)
    gap_x = jnp.minimum(along_x, NX - along_x) / CX
    gap_y = jnp.minimum(along_y, NY - along_y) / CY
    bump = jnp.exp(-0.5 * (gap_x[:, None] * gap_x[:, None] + gap_y[None, :] * gap_y[None, :]))
    return noise * (0.5 + 8.0 * bump)


def block_levels(key, dims, pieces, smallest, top_value):
    def one(dim, parts):
        draws = jax.random.uniform(jax.random.fold_in(jax.random.fold_in(key, 6), dim), (parts,), jnp.float32, smallest / len(pieces), top_value / len(pieces))
        return jnp.repeat(jnp.exp(draws), dims[dim] // parts).reshape((-1,) + (1,) * (len(dims) - dim - 1))

    gain = one(*pieces[0])
    for cut in pieces[1:]:
        gain = gain * one(*cut)
    return gain


def scatter_about(stream_key, extent, deviation, limit, split=(), held_as=jnp.bfloat16):
    loudness = block_levels(stream_key, extent, split, -0.22, 0.18) if split else 1.0
    drawn = jax.random.normal(stream_key, extent, jnp.float32) * deviation * loudness
    return jnp.minimum(jnp.maximum(drawn, -limit), limit).astype(held_as)


def setup_inputs(seed: int = 0) -> dict:
    arg_keys = jax.random.split(jax.random.key(seed), 6)
    return {
        "right_side": draw_right_side(jax.random.fold_in(arg_keys[5], 71), 0),
        "initial": scatter_about(arg_keys[1], (NX, NY), 0.1, 0.6, ((0, 2), (1, 64)), jnp.float32),
        "reaction": jnp.clip(jnp.exp(math.log(0.5) - 2.3025851 * jax.random.uniform(arg_keys[2], (NX, NY), jnp.float32) ** block_levels(arg_keys[2], (NX, NY), ((0, 2), (1, 64)), -0.2, 0.2)), 0.05, 0.5),
        "velocity_x": jnp.clip(jax.random.uniform(arg_keys[3], (NX, NY), jnp.float32, -1.0, 1.0) * block_levels(arg_keys[3], (NX, NY), ((0, 2), (1, 64)), -0.4, 0.0), -1.0, 1.0),
        "velocity_y": jnp.clip(jax.random.uniform(arg_keys[4], (NX, NY), jnp.float32, -1.0, 1.0) * block_levels(arg_keys[4], (NX, NY), ((0, 2), (1, 64)), -0.4, 0.0), -1.0, 1.0),
    }


def moved(field, offset, dimension):
    return jnp.roll(field, -offset, dimension)

def first_diff(field, dimension):
    outer = moved(field, -2, dimension) - moved(field, 2, dimension)
    inner = moved(field, 1, dimension) - moved(field, -1, dimension)
    return (outer + 8.0 * inner) / 12.0

def second_diff(field, dimension):
    inner = moved(field, 1, dimension) + moved(field, -1, dimension)
    outer = moved(field, 2, dimension) + moved(field, -2, dimension)
    return (16.0 * inner - outer - 30.0 * field) / 12.0

def operate(field, reaction, velocity_x, velocity_y):
    diffusion = second_diff(field, 0) + second_diff(field, 1)
    advect_x = 0.5 * (velocity_x * first_diff(field, 0) + first_diff(velocity_x * field, 0))
    advect_y = 0.5 * (velocity_y * first_diff(field, 1) + first_diff(velocity_y * field, 1))
    return reaction * field - diffusion + advect_x + advect_y

def least_squares(hessenberg, beta):
    columns_total = hessenberg.shape[1]
    target = jnp.where(jnp.arange(columns_total + 1) == 0, beta, 0.0)

    def rotate(column, carried):
        upper, target = carried
        top_row = upper[column]
        next_row = upper[column + 1]
        diagonal_entry = top_row[column]
        below_entry = next_row[column]
        radius = jnp.sqrt(diagonal_entry * diagonal_entry + below_entry * below_entry)
        cosine = diagonal_entry / radius
        sine_value = below_entry / radius
        upper = upper.at[column].set(cosine * top_row + sine_value * next_row)
        upper = upper.at[column + 1].set(cosine * next_row - sine_value * top_row)
        upper_value = target[column]
        lower_value = target[column + 1]
        target = target.at[column].set(cosine * upper_value + sine_value * lower_value)
        target = target.at[column + 1].set(cosine * lower_value - sine_value * upper_value)
        return (upper, target)
    upper, target = lax.fori_loop(0, columns_total, rotate, (hessenberg, target))

    def substitute(count, weights):
        row_index = columns_total - 1 - count
        known = jnp.sum(upper[row_index] * weights)
        return weights.at[row_index].set((target[row_index] - known) / upper[row_index, row_index])
    return lax.fori_loop(0, columns_total, substitute, jnp.zeros((columns_total,), jnp.float32))

def reference(right_side, initial, reaction, velocity_x, velocity_y):

    def operator_on(field):
        return operate(field, reaction, velocity_x, velocity_y)
    start_residual = right_side - operator_on(initial)
    beta = jnp.sqrt(jnp.sum(start_residual * start_residual))
    basis = [start_residual / beta]
    hessenberg = jnp.zeros((RESTART + 1, RESTART), jnp.float32)
    for column in range(RESTART):
        applied = operator_on(basis[column])
        projection = jnp.stack([jnp.sum(vector * applied) for vector in basis])
        correction = jnp.zeros_like(applied)
        for position, vector in enumerate(basis):
            correction = correction + projection[position] * vector
        applied = applied - correction
        length = jnp.sqrt(jnp.sum(applied * applied))
        hessenberg = hessenberg.at[:column + 1, column].set(projection)
        hessenberg = hessenberg.at[column + 1, column].set(length)
        basis.append(applied / length)
    weights = least_squares(hessenberg, beta)
    solution = initial
    for position in range(RESTART):
        solution = solution + weights[position] * basis[position]
    residual = right_side - operator_on(solution)
    return (solution, residual)
```

```python
import functools

import jax
import jax.numpy as jnp
from jax import lax
from jax.experimental import pallas as pl
from jax.experimental.pallas import tpu as pltpu
from jax.sharding import Mesh
from jax.sharding import PartitionSpec as P

RESTART = 15
GY = ("gy_0", "gy_1", "gy_2")
ALL = ("gx",) + GY
FIELDS = 5
ROWS, COLS, LANES, HALO = 64, 256, 128, 32
FULL = 2 * ROWS
CENTRE, SPREAD, SHRINK = 5.8, 5.0, 0.9
SCALE = 2.0 * SHRINK / SPREAD
ALPHA = SCALE * CENTRE
SQUARE = SHRINK * SHRINK


def lane_group():
    return lax.broadcasted_iota(jnp.int32, (1, LANES), 1) // HALO


def packed_edges(tiles, lane):
    group = lane_group()
    top, bottom = None, None
    for q in range(4):
        shift = (HALO * q - lane) % LANES
        moved = pltpu.roll(tiles[q], shift, 1) if shift else tiles[q]
        part = tiles[4][16 * q : 16 * q + 16]
        part = pltpu.roll(part, shift, 1) if shift else part
        top = moved if q == 0 else jnp.where(group == q, moved, top)
        bottom = part if q == 0 else jnp.where(group == q, part, bottom)
    return top, bottom


def unpacked_edges(ref, base, lane):
    top = ref[base : base + ROWS, :]
    bottom = ref[base + ROWS : base + ROWS + 16, :]
    tiles, parts = [], []
    for q in range(4):
        shift = (lane - HALO * q) % LANES
        tiles.append(pltpu.roll(top, shift, 1) if shift else top)
        parts.append(pltpu.roll(bottom, shift, 1) if shift else bottom)
    return tiles + [jnp.concatenate(parts, axis=0)]


def pack_body(core_ref, *refs):
    fields, (partner_ref, cross_ref, same_ref) = refs[:FIELDS], refs[FIELDS:]

    def put(ref, base, edges):
        ref[base : base + ROWS, :] = edges[0]
        ref[base + ROWS : base + ROWS + 16, :] = edges[1]

    for core in (0, 1):

        @pl.when(core_ref[0] == core)
        def _():
            left = [f[:, :LANES] for f in fields]
            right = [f[:, LANES:] for f in fields]
            give, keep = (right, left) if core == 0 else (left, right)
            for a in range(FIELDS):
                partner_ref[ROWS * a : ROWS * (a + 1), :] = give[a]
            put(partner_ref, FIELDS * ROWS, packed_edges(keep, 96 if core == 0 else 0))
            left_edge, right_edge = packed_edges(left, 0), packed_edges(right, 96)
            put(cross_ref, 0, left_edge if core == 0 else right_edge)
            put(same_ref, 0, right_edge if core == 0 else left_edge)


def basis_body(core_ref, *refs):
    fields = refs[:FIELDS]
    partner_ref, cross_ref, same_ref, own_ref, give_ref, gram_ref = refs[FIELDS : FIELDS + 6]
    data, coef, basis, image, pairs = refs[FIELDS + 6 :]
    lane = lax.broadcasted_iota(jnp.int32, (1, LANES), 1)

    for core in (0, 1):

        @pl.when(core_ref[0] == core)
        def _():
            mine, beside = (slice(0, LANES), slice(LANES, COLS))
            if core:
                mine, beside = beside, mine
            far = 96 if core == 0 else 0
            near = 96 - far
            same = unpacked_edges(same_ref, 0, far)
            cross = unpacked_edges(cross_ref, 0, far)
            inner = unpacked_edges(partner_ref, FIELDS * ROWS, near)
            for a in range(FIELDS):
                data[a, 8 : 8 + ROWS, :LANES] = fields[a][:, mine]
                data[a, 8 + ROWS : 8 + FULL, :LANES] = partner_ref[ROWS * a : ROWS * (a + 1), :]
                for row, here, there in ((8, fields[a][:, beside], same[a]), (8 + ROWS, inner[a], cross[a])):
                    low, high = (here, there) if core == 0 else (there, here)
                    tile = jnp.where(lane < HALO, low, jnp.where(lane >= LANES - HALO, high, 0.0))
                    data[a, row : row + ROWS, LANES:] = tile

    for a in range(FIELDS):
        data[a, 0:8, :] = data[a, FULL : FULL + 8, :]
        data[a, 8 + FULL : 16 + FULL, :] = data[a, 8:16, :]

    for r in range(0, FULL, 16):
        rows = slice(r, r + 16)
        at = lambda a, o: data[a, 8 + r + o : 24 + r + o, :]
        coef[0, rows, :] = SCALE * (at(2, 0) + (5.0 - CENTRE))
        vx, vy = at(3, 0), at(4, 0)
        for o in (1, 2):
            base = SCALE * (-4.0 / 3.0 if o == 1 else 1.0 / 12.0)
            turn = SCALE * (1.0 / 3.0 if o == 1 else -1.0 / 24.0)
            coef[4 * o - 3, rows, :] = base + turn * (vx + at(3, o))
            coef[4 * o - 2, rows, :] = base - turn * (vx + at(3, -o))
            coef[4 * o - 1, rows, :] = base + turn * (vy + pltpu.roll(vy, COLS - o, 1))
            coef[4 * o, rows, :] = base - turn * (vy + pltpu.roll(vy, o, 1))

    def stencil(load, r):
        rows = slice(r, r + 16)
        field = load(0)
        total = coef[0, rows, :] * field
        for o in (1, 2):
            total += coef[4 * o - 3, rows, :] * load(o)
            total += coef[4 * o - 2, rows, :] * load(-o)
            total += coef[4 * o - 1, rows, :] * pltpu.roll(field, COLS - o, 1)
            total += coef[4 * o, rows, :] * pltpu.roll(field, o, 1)
        return field, total

    def wrap(index):
        basis[index, 0:8, :] = basis[index, FULL : FULL + 8, :]
        basis[index, 8 + FULL : 16 + FULL, :] = basis[index, 8:16, :]

    basis[0, 8 : 8 + FULL, :] = jnp.zeros((FULL, COLS), jnp.float32)
    for r in range(0, FULL, 16):
        field, total = stencil(lambda o: data[1, 8 + r + o : 24 + r + o, :], r)
        start = data[0, 8 + r : 24 + r, :] - ((1.0 / SCALE) * total + CENTRE * field)
        basis[1, 8 + r : 24 + r, :] = start
        image[RESTART, r : r + 16, :] = start[:, :LANES]
    wrap(1)

    def step(j, carried):
        for r in range(0, FULL, 16):
            field, total = stencil(lambda o: basis[j + 1, 8 + r + o : 24 + r + o, :], r)
            image[j, r : r + 16, :] = total[:, :LANES] + ALPHA * field[:, :LANES]
            basis[j + 2, 8 + r : 24 + r, :] = total - SQUARE * basis[j, 8 + r : 24 + r, :]
        wrap(j + 2)
        return carried

    lax.fori_loop(0, RESTART, step, 0)
    own_ref[...] = basis[1:, 8 : 8 + ROWS, :LANES]
    give_ref[...] = basis[1:, 8 + ROWS : 8 + FULL, :LANES]

    for low in range(0, 16, 4):
        for high in range(low, 16, 4):

            def accumulate(t, sums):
                rows = pl.ds(pl.multiple_of(8 * t, 8), 8)
                first = [image[low + i, rows, :] for i in range(4)]
                second = first if low == high else [image[high + i, rows, :] for i in range(4)]
                return tuple(sums[4 * i + k] + first[i] * second[k] for i in range(4) for k in range(4))

            sums = lax.fori_loop(
                0, FULL // 8, accumulate, tuple(jnp.zeros((8, LANES), jnp.float32) for _ in range(16)), unroll=2
            )
            for i in range(4):
                for k in range(4):
                    row = jnp.sum(sums[4 * i + k], axis=0, keepdims=True)
                    at = 16 * (low + i) + high + k
                    pairs[at : at + 1, :] = row
                    if low != high:
                        at = 16 * (high + k) + low + i
                        pairs[at : at + 1, :] = row
    total = lax.dot_general(
        jnp.ones((8, LANES), jnp.float32),
        pairs[...],
        (((1,), (1,)), ((), ())),
        precision=lax.Precision.HIGHEST,
        preferred_element_type=jnp.float32,
    )
    gram_ref[...] = total


def finish_body(core_ref, sums_ref, partner_sums_ref, own_ref, got_ref, initial_ref, solution_ref, residual_ref):
    total = jnp.sum(sums_ref[...] + partner_sums_ref[...], axis=0)
    total = jnp.concatenate([total[0:1], total[1:2]], axis=1)
    lane = lax.broadcasted_iota(jnp.int32, (16, COLS), 1)
    sub = lax.broadcasted_iota(jnp.int32, (16, COLS), 0)
    spread = jnp.where(lane // 16 == sub, total, 0.0)
    pick_row = lax.broadcasted_iota(jnp.int32, (COLS, LANES), 0) % 16
    pick_col = lax.broadcasted_iota(jnp.int32, (COLS, LANES), 1)
    pick = jnp.where(pick_row == pick_col, 1.0, 0.0)
    gram = jnp.dot(spread, pick, precision=lax.Precision.HIGHEST, preferred_element_type=jnp.float32)
    columns = [jnp.broadcast_to(gram[:, k : k + 1], (16, LANES)) for k in range(16)]
    row_at = lax.broadcasted_iota(jnp.int32, (16, LANES), 0)
    for k in range(RESTART):
        inverse = 1.0 / columns[k][k : k + 1, :]
        for j in range(k + 1, 16):
            top = columns[j][k : k + 1, :] * inverse
            columns[j] = jnp.where(row_at == k, top, columns[j] - columns[k] * top)
    z = [columns[RESTART][k : k + 1, :] for k in range(RESTART)]
    left = []
    for k in range(16):
        value = 1.0 if k == 0 else 0.0
        if k > 0:
            value = value - z[k - 1]
        if k < RESTART:
            value = value - ALPHA * z[k]
        if k + 1 < RESTART:
            value = value - SQUARE * z[k + 1]
        left.append(value)
    step = [SCALE * z[k] for k in range(RESTART)]
    first = core_ref[0] == 0
    for r in range(0, ROWS, 8):
        rows = slice(r, r + 8)
        sums = []
        for ref in (own_ref, got_ref):
            change, rest = None, None
            for k in range(16):
                vector = ref[k, rows, :]
                rest = left[k] * vector if k == 0 else rest + left[k] * vector
                if k < RESTART:
                    change = step[k] * vector if k == 0 else change + step[k] * vector
            sums.append((change, rest))
        (own_change, own_rest), (got_change, got_rest) = sums
        solution_ref[rows, :LANES] = initial_ref[rows, :LANES] + jnp.where(first, own_change, got_change)
        solution_ref[rows, LANES:] = initial_ref[rows, LANES:] + jnp.where(first, got_change, own_change)
        residual_ref[rows, :LANES] = jnp.where(first, own_rest, got_rest)
        residual_ref[rows, LANES:] = jnp.where(first, got_rest, own_rest)


def call(body, out_shape, n_in, scratch=(), name=None):
    vmem = pl.BlockSpec(memory_space=pltpu.VMEM)
    return pl.pallas_call(
        body,
        out_shape=out_shape,
        in_specs=[pl.BlockSpec(memory_space=pltpu.SMEM)] + [vmem] * n_in,
        out_specs=jax.tree.map(lambda _: vmem, out_shape),
        scratch_shapes=scratch,
        name=name,
    )


def f32(*shape):
    return jax.ShapeDtypeStruct(shape, jnp.float32)


def per_device(right_side, initial, reaction, velocity_x, velocity_y):
    fields = (right_side, initial, reaction, velocity_x, velocity_y)
    core = lax.axis_index("gx").astype(jnp.int32).reshape(1)
    count = lax.axis_size(GY)
    swap = [(0, 1), (1, 0)]
    ahead = lambda g: (g + 1) % count
    behind = lambda g: (g - 1) % count
    cross = [(g, count + behind(g)) for g in range(count)] + [(count + g, ahead(g)) for g in range(count)]
    same = [(g, ahead(g)) for g in range(count)] + [(count + g, count + behind(g)) for g in range(count)]

    edge = f32(ROWS + 16, LANES)
    to_partner, to_cross, to_same = call(
        pack_body, (f32(FIELDS * ROWS + ROWS + 16, LANES), edge, edge), FIELDS, name="pack"
    )(core, *fields)
    from_partner = lax.ppermute(to_partner, "gx", swap)
    from_cross = lax.ppermute(to_cross, ALL, cross)
    from_same = lax.ppermute(to_same, ALL, same)
    own, give, gram = call(
        basis_body,
        (f32(16, ROWS, LANES), f32(16, ROWS, LANES), f32(8, COLS)),
        FIELDS + 3,
        scratch=[
            pltpu.VMEM((FIELDS, FULL + 16, COLS), jnp.float32),
            pltpu.VMEM((9, FULL, COLS), jnp.float32),
            pltpu.VMEM((RESTART + 2, FULL + 16, COLS), jnp.float32),
            pltpu.VMEM((16, FULL, LANES), jnp.float32),
            pltpu.VMEM((COLS, LANES), jnp.float32),
        ],
        name="basis",
    )(core, *fields, from_partner, from_cross, from_same)
    got = lax.ppermute(give, "gx", swap)
    gram = gram[0].reshape(1, 2, LANES)
    sums = lax.all_to_all(jnp.broadcast_to(gram, (count, 2, LANES)), GY, 0, 0, tiled=True)
    partner_sums = lax.ppermute(sums, "gx", swap)
    return call(finish_body, (f32(ROWS, COLS), f32(ROWS, COLS)), 5, name="finish")(
        core, sums, partner_sums, own, got, initial
    )


def solution(mesh):
    torus = Mesh(mesh.devices.reshape(mesh.shape["gx"], 4, 4, 4), ALL)
    placed = P("gx", GY)
    return jax.shard_map(
        per_device,
        mesh=torus,
        in_specs=(placed,) * FIELDS,
        out_specs=(placed, placed),
        check_vma=False,
    )
```

```python
import functools

import jax
import jax.numpy as jnp
from jax import lax
from jax.experimental import pallas as pl
from jax.experimental.pallas import tpu as pltpu
from jax.sharding import Mesh
from jax.sharding import PartitionSpec as P

RESTART = 15
GY = ("gy_0", "gy_1", "gy_2")
ALL = ("gx",) + GY
FIELDS = 5
ROWS, COLS, LANES, HALO = 64, 256, 128, 32
FULL = 2 * ROWS
CENTRE, SPREAD, SHRINK = 5.8, 5.0, 0.9
SCALE = 2.0 * SHRINK / SPREAD
ALPHA = SCALE * CENTRE
SQUARE = SHRINK * SHRINK


def lane_group():
    return lax.broadcasted_iota(jnp.int32, (1, LANES), 1) // HALO


def packed_edges(tiles, lane):
    group = lane_group()
    top, bottom = None, None
    for q in range(4):
        shift = (HALO * q - lane) % LANES
        moved = pltpu.roll(tiles[q], shift, 1) if shift else tiles[q]
        part = tiles[4][16 * q : 16 * q + 16]
        part = pltpu.roll(part, shift, 1) if shift else part
        top = moved if q == 0 else jnp.where(group == q, moved, top)
        bottom = part if q == 0 else jnp.where(group == q, part, bottom)
    return top, bottom


def unpacked_edges(ref, base, lane):
    top = ref[base : base + ROWS, :]
    bottom = ref[base + ROWS : base + ROWS + 16, :]
    tiles, parts = [], []
    for q in range(4):
        shift = (lane - HALO * q) % LANES
        tiles.append(pltpu.roll(top, shift, 1) if shift else top)
        parts.append(pltpu.roll(bottom, shift, 1) if shift else bottom)
    return tiles + [jnp.concatenate(parts, axis=0)]


def pack_body(core_ref, *refs):
    fields, (same_ref, cross_ref, partner_ref, held_ref) = refs[:FIELDS], refs[FIELDS:]
    for a in range(FIELDS):
        held_ref[a] = fields[a][...]

    def put(ref, base, edges):
        ref[base : base + ROWS, :] = edges[0]
        ref[base + ROWS : base + ROWS + 16, :] = edges[1]

    for core in (0, 1):

        @pl.when(core_ref[0] == core)
        def _():
            left = [f[:, :LANES] for f in fields]
            right = [f[:, LANES:] for f in fields]
            give, keep = (right, left) if core == 0 else (left, right)
            for a in range(FIELDS):
                partner_ref[ROWS * a : ROWS * (a + 1), :] = give[a]
            put(partner_ref, FIELDS * ROWS, packed_edges(keep, 96 if core == 0 else 0))
            left_edge, right_edge = packed_edges(left, 0), packed_edges(right, 96)
            put(cross_ref, 0, left_edge if core == 0 else right_edge)
            put(same_ref, 0, right_edge if core == 0 else left_edge)


def basis_body(core_ref, *refs):
    held_ref, partner_ref, cross_ref, same_ref, own_ref, give_ref, gram_ref = refs[:7]
    data, coef, basis, image, pairs = refs[7:]
    lane = lax.broadcasted_iota(jnp.int32, (1, LANES), 1)

    for core in (0, 1):

        @pl.when(core_ref[0] == core)
        def _():
            mine, beside = (slice(0, LANES), slice(LANES, COLS))
            if core:
                mine, beside = beside, mine
            far = 96 if core == 0 else 0
            near = 96 - far
            same = unpacked_edges(same_ref, 0, far)
            cross = unpacked_edges(cross_ref, 0, far)
            inner = unpacked_edges(partner_ref, FIELDS * ROWS, near)
            for a in range(FIELDS):
                data[a, 8 : 8 + ROWS, :LANES] = held_ref[a, :, mine]
                data[a, 8 + ROWS : 8 + FULL, :LANES] = partner_ref[ROWS * a : ROWS * (a + 1), :]
                for row, here, there in ((8, held_ref[a, :, beside], same[a]), (8 + ROWS, inner[a], cross[a])):
                    low, high = (here, there) if core == 0 else (there, here)
                    tile = jnp.where(lane < HALO, low, jnp.where(lane >= LANES - HALO, high, 0.0))
                    data[a, row : row + ROWS, LANES:] = tile

    for a in range(FIELDS):
        data[a, 0:8, :] = data[a, FULL : FULL + 8, :]
        data[a, 8 + FULL : 16 + FULL, :] = data[a, 8:16, :]

    for r in range(0, FULL, 16):
        rows = slice(r, r + 16)
        at = lambda a, o: data[a, 8 + r + o : 24 + r + o, :]
        coef[0, rows, :] = SCALE * (at(2, 0) + (5.0 - CENTRE))
        vx, vy = at(3, 0), at(4, 0)
        for o in (1, 2):
            base = SCALE * (-4.0 / 3.0 if o == 1 else 1.0 / 12.0)
            turn = SCALE * (1.0 / 3.0 if o == 1 else -1.0 / 24.0)
            coef[4 * o - 3, rows, :] = base + turn * (vx + at(3, o))
            coef[4 * o - 2, rows, :] = base - turn * (vx + at(3, -o))
            coef[4 * o - 1, rows, :] = base + turn * (vy + pltpu.roll(vy, COLS - o, 1))
            coef[4 * o, rows, :] = base - turn * (vy + pltpu.roll(vy, o, 1))

    def stencil(load, r):
        rows = slice(r, r + 16)
        field = load(0)
        total = coef[0, rows, :] * field
        for o in (1, 2):
            total += coef[4 * o - 3, rows, :] * load(o)
            total += coef[4 * o - 2, rows, :] * load(-o)
            total += coef[4 * o - 1, rows, :] * pltpu.roll(field, COLS - o, 1)
            total += coef[4 * o, rows, :] * pltpu.roll(field, o, 1)
        return field, total

    def wrap(index):
        basis[index, 0:8, :] = basis[index, FULL : FULL + 8, :]
        basis[index, 8 + FULL : 16 + FULL, :] = basis[index, 8:16, :]

    basis[0, 8 : 8 + FULL, :] = jnp.zeros((FULL, COLS), jnp.float32)
    for r in range(0, FULL, 16):
        field, total = stencil(lambda o: data[1, 8 + r + o : 24 + r + o, :], r)
        start = data[0, 8 + r : 24 + r, :] - ((1.0 / SCALE) * total + CENTRE * field)
        basis[1, 8 + r : 24 + r, :] = start
        image[RESTART, r : r + 16, :] = start[:, :LANES]
    wrap(1)

    def step(j, carried):
        for r in range(0, FULL, 16):
            field, total = stencil(lambda o: basis[j + 1, 8 + r + o : 24 + r + o, :], r)
            image[j, r : r + 16, :] = total[:, :LANES] + ALPHA * field[:, :LANES]
            basis[j + 2, 8 + r : 24 + r, :] = total - SQUARE * basis[j, 8 + r : 24 + r, :]
        wrap(j + 2)
        return carried

    lax.fori_loop(0, RESTART, step, 0)
    own_ref[...] = basis[1:, 8 : 8 + ROWS, :LANES]
    give_ref[...] = basis[1:, 8 + ROWS : 8 + FULL, :LANES]

    for low in range(0, 16, 4):
        for high in range(low, 16, 4):

            def accumulate(t, sums):
                rows = pl.ds(pl.multiple_of(8 * t, 8), 8)
                first = [image[low + i, rows, :] for i in range(4)]
                second = first if low == high else [image[high + i, rows, :] for i in range(4)]
                return tuple(sums[4 * i + k] + first[i] * second[k] for i in range(4) for k in range(4))

            sums = lax.fori_loop(
                0, FULL // 8, accumulate, tuple(jnp.zeros((8, LANES), jnp.float32) for _ in range(16)), unroll=2
            )
            for i in range(4):
                for k in range(4):
                    row = jnp.sum(sums[4 * i + k], axis=0, keepdims=True)
                    at = 16 * (low + i) + high + k
                    pairs[at : at + 1, :] = row
                    if low != high:
                        at = 16 * (high + k) + low + i
                        pairs[at : at + 1, :] = row
    total = lax.dot_general(
        jnp.ones((8, LANES), jnp.float32),
        pairs[...],
        (((1,), (1,)), ((), ())),
        precision=lax.Precision.HIGHEST,
        preferred_element_type=jnp.float32,
    )
    both = jnp.concatenate([total[0:1, :LANES], total[0:1, LANES:]], axis=0)
    gram_ref[...] = jnp.broadcast_to(both[None], gram_ref.shape)


def finish_body(core_ref, sums_ref, own_ref, got_ref, held_ref, solution_ref, residual_ref):
    total = jnp.sum(sums_ref[...], axis=0)
    total = jnp.concatenate([total[0:1], total[1:2]], axis=1)
    lane = lax.broadcasted_iota(jnp.int32, (16, COLS), 1)
    sub = lax.broadcasted_iota(jnp.int32, (16, COLS), 0)
    spread = jnp.where(lane // 16 == sub, total, 0.0)
    pick_row = lax.broadcasted_iota(jnp.int32, (COLS, LANES), 0) % 16
    pick_col = lax.broadcasted_iota(jnp.int32, (COLS, LANES), 1)
    pick = jnp.where(pick_row == pick_col, 1.0, 0.0)
    gram = jnp.dot(spread, pick, precision=lax.Precision.HIGHEST, preferred_element_type=jnp.float32)
    columns = [jnp.broadcast_to(gram[:, k : k + 1], (16, LANES)) for k in range(16)]
    row_at = lax.broadcasted_iota(jnp.int32, (16, LANES), 0)
    for k in range(RESTART):
        inverse = 1.0 / columns[k][k : k + 1, :]
        for j in range(k + 1, 16):
            top = columns[j][k : k + 1, :] * inverse
            columns[j] = jnp.where(row_at == k, top, columns[j] - columns[k] * top)
    z = [columns[RESTART][k : k + 1, :] for k in range(RESTART)]
    left = []
    for k in range(16):
        value = 1.0 if k == 0 else 0.0
        if k > 0:
            value = value - z[k - 1]
        if k < RESTART:
            value = value - ALPHA * z[k]
        if k + 1 < RESTART:
            value = value - SQUARE * z[k + 1]
        left.append(value)
    step = [SCALE * z[k] for k in range(RESTART)]
    first = core_ref[0] == 0
    for r in range(0, ROWS, 8):
        rows = slice(r, r + 8)
        sums = []
        for ref in (own_ref, got_ref):
            change, rest = None, None
            for k in range(16):
                vector = ref[k, rows, :]
                rest = left[k] * vector if k == 0 else rest + left[k] * vector
                if k < RESTART:
                    change = step[k] * vector if k == 0 else change + step[k] * vector
            sums.append((change, rest))
        (own_change, own_rest), (got_change, got_rest) = sums
        solution_ref[rows, :LANES] = held_ref[1, rows, :LANES] + jnp.where(first, own_change, got_change)
        solution_ref[rows, LANES:] = held_ref[1, rows, LANES:] + jnp.where(first, got_change, own_change)
        residual_ref[rows, :LANES] = jnp.where(first, own_rest, got_rest)
        residual_ref[rows, LANES:] = jnp.where(first, got_rest, own_rest)


def call(body, out_shape, scratch=(), name=None, staged=True):
    vmem = pl.BlockSpec(memory_space=pltpu.VMEM)

    def run(core, *args):
        if staged:
            args = [pltpu.with_memory_space_constraint(a, pltpu.VMEM) for a in args]
        return pl.pallas_call(
            body,
            out_shape=out_shape,
            in_specs=[pl.BlockSpec(memory_space=pltpu.SMEM)] + [vmem] * len(args),
            out_specs=tuple(vmem for _ in out_shape),
            scratch_shapes=scratch,
            name=name,
        )(core, *args)

    return run


def on_chip(*shape):
    return pltpu.VMEM(shape, jnp.float32)


def per_device(right_side, initial, reaction, velocity_x, velocity_y):
    fields = (right_side, initial, reaction, velocity_x, velocity_y)
    core = lax.axis_index("gx").astype(jnp.int32).reshape(1)
    count = lax.axis_size(GY)
    swap = [(0, 1), (1, 0)]
    ahead = lambda g: (g + 1) % count
    behind = lambda g: (g - 1) % count
    cross = [(g, count + behind(g)) for g in range(count)] + [(count + g, ahead(g)) for g in range(count)]
    same = [(g, ahead(g)) for g in range(count)] + [(count + g, count + behind(g)) for g in range(count)]

    edge = on_chip(ROWS + 16, LANES)
    to_same, to_cross, to_partner, held = call(
        pack_body,
        (edge, edge, on_chip(FIELDS * ROWS + ROWS + 16, LANES), on_chip(FIELDS, ROWS, COLS)),
        name="pack",
        staged=False,
    )(core, *fields)
    from_same = lax.ppermute(to_same, ALL, same)
    from_cross = lax.ppermute(to_cross, ALL, cross)
    from_partner = lax.ppermute(to_partner, "gx", swap)
    own, give, gram = call(
        basis_body,
        (on_chip(16, ROWS, LANES), on_chip(16, ROWS, LANES), on_chip(2 * count, 2, LANES)),
        scratch=[
            on_chip(FIELDS, FULL + 16, COLS),
            on_chip(9, FULL, COLS),
            on_chip(RESTART + 2, FULL + 16, COLS),
            on_chip(16, FULL, LANES),
            on_chip(COLS, LANES),
        ],
        name="basis",
    )(core, held, from_partner, from_cross, from_same)
    got = lax.ppermute(give, "gx", swap)
    sums = lax.all_to_all(gram, ALL, 0, 0, tiled=True)
    result = jax.ShapeDtypeStruct((ROWS, COLS), jnp.float32)
    return call(finish_body, (result, result), name="finish")(core, sums, own, got, held)


def solution(mesh):
    torus = Mesh(mesh.devices.reshape(mesh.shape["gx"], 4, 4, 4), ALL)
    placed = P("gx", GY)
    return jax.shard_map(
        per_device,
        mesh=torus,
        in_specs=(placed,) * FIELDS,
        out_specs=(placed, placed),
        check_vma=False,
    )
```

```python
import jax
import jax.numpy as jnp
from jax import lax
from jax.experimental import pallas as pl
from jax.experimental.pallas import tpu as pltpu
from jax.sharding import Mesh
from jax.sharding import PartitionSpec as P


RESTART = 15
GY = ("gy_0", "gy_1", "gy_2")
ALL = ("gx",) + GY
FIELDS = 5
ROWS, COLS, LANES, HALO = 64, 256, 128, 32
FULL = 2 * ROWS
CENTRE, SPREAD, SHRINK = 5.8, 5.0, 0.9
SCALE = 2.0 * SHRINK / SPREAD
ALPHA = SCALE * CENTRE
SQUARE = SHRINK * SHRINK


def lane_group():
    return lax.broadcasted_iota(jnp.int32, (1, LANES), 1) // HALO


def packed_edges(tiles, lane):
    group = lane_group()
    top, bottom = None, None
    for q in range(4):
        shift = (HALO * q - lane) % LANES
        moved = pltpu.roll(tiles[q], shift, 1) if shift else tiles[q]
        part = tiles[4][16 * q : 16 * q + 16]
        part = pltpu.roll(part, shift, 1) if shift else part
        top = moved if q == 0 else jnp.where(group == q, moved, top)
        bottom = part if q == 0 else jnp.where(group == q, part, bottom)
    return top, bottom


def unpacked_edges(ref, base, lane):
    top = ref[base : base + ROWS, :]
    bottom = ref[base + ROWS : base + ROWS + 16, :]
    tiles, parts = [], []
    for q in range(4):
        shift = (lane - HALO * q) % LANES
        tiles.append(pltpu.roll(top, shift, 1) if shift else top)
        parts.append(pltpu.roll(bottom, shift, 1) if shift else bottom)
    return tiles + [jnp.concatenate(parts, axis=0)]


def pack_body(core_ref, *refs):
    fields, (same_ref, cross_ref, partner_ref, held_ref) = refs[:FIELDS], refs[FIELDS:]
    for a in range(FIELDS):
        held_ref[a] = fields[a][...]

    def put(ref, base, edges):
        ref[base : base + ROWS, :] = edges[0]
        ref[base + ROWS : base + ROWS + 16, :] = edges[1]

    for core in (0, 1):

        @pl.when(core_ref[0] == core)
        def _():
            left = [f[:, :LANES] for f in fields]
            right = [f[:, LANES:] for f in fields]
            give, keep = (right, left) if core == 0 else (left, right)
            for a in range(FIELDS):
                partner_ref[ROWS * a : ROWS * (a + 1), :] = give[a]
            put(partner_ref, FIELDS * ROWS, packed_edges(keep, 96 if core == 0 else 0))
            left_edge, right_edge = packed_edges(left, 0), packed_edges(right, 96)
            put(cross_ref, 0, left_edge if core == 0 else right_edge)
            put(same_ref, 0, right_edge if core == 0 else left_edge)


def basis_body(core_ref, *refs):
    held_ref, partner_ref, cross_ref, same_ref, own_ref, give_ref, gram_ref = refs[:7]
    data, coef, basis, image, pairs = refs[7:]
    lane = lax.broadcasted_iota(jnp.int32, (1, LANES), 1)

    for core in (0, 1):

        @pl.when(core_ref[0] == core)
        def _():
            mine, beside = (slice(0, LANES), slice(LANES, COLS))
            if core:
                mine, beside = beside, mine
            far = 96 if core == 0 else 0
            near = 96 - far
            same = unpacked_edges(same_ref, 0, far)
            cross = unpacked_edges(cross_ref, 0, far)
            inner = unpacked_edges(partner_ref, FIELDS * ROWS, near)
            for a in range(FIELDS):
                data[a, 8 : 8 + ROWS, :LANES] = held_ref[a, :, mine]
                data[a, 8 + ROWS : 8 + FULL, :LANES] = partner_ref[ROWS * a : ROWS * (a + 1), :]
                for row, here, there in ((8, held_ref[a, :, beside], same[a]), (8 + ROWS, inner[a], cross[a])):
                    low, high = (here, there) if core == 0 else (there, here)
                    tile = jnp.where(lane < HALO, low, jnp.where(lane >= LANES - HALO, high, 0.0))
                    data[a, row : row + ROWS, LANES:] = tile

    for a in range(FIELDS):
        data[a, 0:8, :] = data[a, FULL : FULL + 8, :]
        data[a, 8 + FULL : 16 + FULL, :] = data[a, 8:16, :]

    for r in range(0, FULL, 16):
        rows = slice(r, r + 16)
        at = lambda a, o: data[a, 8 + r + o : 24 + r + o, :]
        coef[0, rows, :] = SCALE * (at(2, 0) + (5.0 - CENTRE))
        vx, vy = at(3, 0), at(4, 0)
        for o in (1, 2):
            base = SCALE * (-4.0 / 3.0 if o == 1 else 1.0 / 12.0)
            turn = SCALE * (1.0 / 3.0 if o == 1 else -1.0 / 24.0)
            coef[4 * o - 3, rows, :] = base + turn * (vx + at(3, o))
            coef[4 * o - 2, rows, :] = base - turn * (vx + at(3, -o))
            coef[4 * o - 1, rows, :] = base + turn * (vy + pltpu.roll(vy, COLS - o, 1))
            coef[4 * o, rows, :] = base - turn * (vy + pltpu.roll(vy, o, 1))

    def stencil(load, r):
        rows = slice(r, r + 16)
        field = load(0)
        total = coef[0, rows, :] * field
        for o in (1, 2):
            total += coef[4 * o - 3, rows, :] * load(o)
            total += coef[4 * o - 2, rows, :] * load(-o)
            total += coef[4 * o - 1, rows, :] * pltpu.roll(field, COLS - o, 1)
            total += coef[4 * o, rows, :] * pltpu.roll(field, o, 1)
        return field, total

    def wrap(index):
        basis[index, 0:8, :] = basis[index, FULL : FULL + 8, :]
        basis[index, 8 + FULL : 16 + FULL, :] = basis[index, 8:16, :]

    basis[0, 8 : 8 + FULL, :] = jnp.zeros((FULL, COLS), jnp.float32)
    for r in range(0, FULL, 16):
        field, total = stencil(lambda o: data[1, 8 + r + o : 24 + r + o, :], r)
        start = data[0, 8 + r : 24 + r, :] - ((1.0 / SCALE) * total + CENTRE * field)
        basis[1, 8 + r : 24 + r, :] = start
        image[RESTART, r : r + 16, :] = start[:, :LANES]
    wrap(1)

    def step(j, carried):
        for r in range(0, FULL, 16):
            field, total = stencil(lambda o: basis[j + 1, 8 + r + o : 24 + r + o, :], r)
            image[j, r : r + 16, :] = total[:, :LANES] + ALPHA * field[:, :LANES]
            basis[j + 2, 8 + r : 24 + r, :] = total - SQUARE * basis[j, 8 + r : 24 + r, :]
        wrap(j + 2)
        return carried

    lax.fori_loop(0, RESTART, step, 0)
    own_ref[...] = basis[1:, 8 : 8 + ROWS, :LANES]
    give_ref[...] = basis[1:, 8 + ROWS : 8 + FULL, :LANES]

    for low in range(0, 16, 4):
        for high in range(low, 16, 4):

            def accumulate(t, sums):
                rows = pl.ds(pl.multiple_of(8 * t, 8), 8)
                first = [image[low + i, rows, :] for i in range(4)]
                second = first if low == high else [image[high + i, rows, :] for i in range(4)]
                return tuple(sums[4 * i + k] + first[i] * second[k] for i in range(4) for k in range(4))

            sums = lax.fori_loop(
                0, FULL // 8, accumulate, tuple(jnp.zeros((8, LANES), jnp.float32) for _ in range(16)), unroll=2
            )
            for i in range(4):
                for k in range(4):
                    row = jnp.sum(sums[4 * i + k], axis=0, keepdims=True)
                    at = 16 * (low + i) + high + k
                    pairs[at : at + 1, :] = row
                    if low != high:
                        at = 16 * (high + k) + low + i
                        pairs[at : at + 1, :] = row
    total = lax.dot_general(
        jnp.ones((8, LANES), jnp.float32),
        pairs[...],
        (((1,), (1,)), ((), ())),
        precision=lax.Precision.HIGHEST,
        preferred_element_type=jnp.float32,
    )
    both = jnp.concatenate([total[0:1, :LANES], total[0:1, LANES:]], axis=0)
    gram_ref[...] = jnp.broadcast_to(both[None], gram_ref.shape)


def finish_body(core_ref, sums_ref, own_ref, got_ref, held_ref, solution_ref, residual_ref):
    total = jnp.sum(sums_ref[...], axis=0)
    total = jnp.concatenate([total[0:1], total[1:2]], axis=1)
    lane = lax.broadcasted_iota(jnp.int32, (16, COLS), 1)
    sub = lax.broadcasted_iota(jnp.int32, (16, COLS), 0)
    spread = jnp.where(lane // 16 == sub, total, 0.0)
    pick_row = lax.broadcasted_iota(jnp.int32, (COLS, LANES), 0) % 16
    pick_col = lax.broadcasted_iota(jnp.int32, (COLS, LANES), 1)
    pick = jnp.where(pick_row == pick_col, 1.0, 0.0)
    gram = jnp.dot(spread, pick, precision=lax.Precision.HIGHEST, preferred_element_type=jnp.float32)
    columns = [jnp.broadcast_to(gram[:, k : k + 1], (16, LANES)) for k in range(16)]
    row_at = lax.broadcasted_iota(jnp.int32, (16, LANES), 0)
    for k in range(RESTART):
        inverse = 1.0 / columns[k][k : k + 1, :]
        for j in range(k + 1, 16):
            top = columns[j][k : k + 1, :] * inverse
            columns[j] = jnp.where(row_at == k, top, columns[j] - columns[k] * top)
    z = [columns[RESTART][k : k + 1, :] for k in range(RESTART)]
    left = []
    for k in range(16):
        value = 1.0 if k == 0 else 0.0
        if k > 0:
            value = value - z[k - 1]
        if k < RESTART:
            value = value - ALPHA * z[k]
        if k + 1 < RESTART:
            value = value - SQUARE * z[k + 1]
        left.append(value)
    step = [SCALE * z[k] for k in range(RESTART)]
    first = core_ref[0] == 0
    for r in range(0, ROWS, 8):
        rows = slice(r, r + 8)
        sums = []
        for ref in (own_ref, got_ref):
            change, rest = None, None
            for k in range(16):
                vector = ref[k, rows, :]
                rest = left[k] * vector if k == 0 else rest + left[k] * vector
                if k < RESTART:
                    change = step[k] * vector if k == 0 else change + step[k] * vector
            sums.append((change, rest))
        (own_change, own_rest), (got_change, got_rest) = sums
        solution_ref[rows, :LANES] = held_ref[1, rows, :LANES] + jnp.where(first, own_change, got_change)
        solution_ref[rows, LANES:] = held_ref[1, rows, LANES:] + jnp.where(first, got_change, own_change)
        residual_ref[rows, :LANES] = jnp.where(first, own_rest, got_rest)
        residual_ref[rows, LANES:] = jnp.where(first, got_rest, own_rest)


def call(body, out_shape, scratch=(), staged=True):
    vmem = pl.BlockSpec(memory_space=pltpu.VMEM)

    def run(core, *args):
        if staged:
            args = [pltpu.with_memory_space_constraint(a, pltpu.VMEM) for a in args]
        return pl.pallas_call(
            body,
            out_shape=out_shape,
            in_specs=[pl.BlockSpec(memory_space=pltpu.SMEM)] + [vmem] * len(args),
            out_specs=tuple(vmem for _ in out_shape),
            scratch_shapes=scratch,
        )(core, *args)

    return run


def on_chip(*shape):
    return pltpu.VMEM(shape, jnp.float32)


def per_device(right_side, initial, reaction, velocity_x, velocity_y):
    fields = (right_side, initial, reaction, velocity_x, velocity_y)
    core = lax.axis_index("gx").astype(jnp.int32).reshape(1)
    count = lax.axis_size(GY)
    swap = [(0, 1), (1, 0)]
    ahead = lambda g: (g + 1) % count
    behind = lambda g: (g - 1) % count
    cross = [(g, count + behind(g)) for g in range(count)] + [(count + g, ahead(g)) for g in range(count)]
    same = [(g, ahead(g)) for g in range(count)] + [(count + g, count + behind(g)) for g in range(count)]

    edge = on_chip(ROWS + 16, LANES)
    to_same, to_cross, to_partner, held = call(
        pack_body, (edge, edge, on_chip(FIELDS * ROWS + ROWS + 16, LANES), on_chip(FIELDS, ROWS, COLS)), staged=False
    )(core, *fields)
    from_same = lax.ppermute(to_same, ALL, same)
    from_cross = lax.ppermute(to_cross, ALL, cross)
    from_partner = lax.ppermute(to_partner, "gx", swap)
    own, give, gram = call(
        basis_body,
        (on_chip(16, ROWS, LANES), on_chip(16, ROWS, LANES), on_chip(2 * count, 2, LANES)),
        scratch=[
            on_chip(FIELDS, FULL + 16, COLS),
            on_chip(9, FULL, COLS),
            on_chip(RESTART + 2, FULL + 16, COLS),
            on_chip(16, FULL, LANES),
            on_chip(COLS, LANES),
        ],
    )(core, held, from_partner, from_cross, from_same)
    got = lax.ppermute(give, "gx", swap)
    sums = lax.all_to_all(gram, ALL, 0, 0, tiled=True)
    result = jax.ShapeDtypeStruct((ROWS, COLS), jnp.float32)
    return call(finish_body, (result, result))(core, sums, own, got, held)


def solution(mesh):
    torus = Mesh(mesh.devices.reshape(mesh.shape["gx"], 4, 4, 4), ALL)
    placed = P("gx", GY)
    return jax.shard_map(
        per_device,
        mesh=torus,
        in_specs=(placed,) * FIELDS,
        out_specs=(placed, placed),
        check_vma=False,
    )
```

```python
import jax
import jax.numpy as jnp
from jax import lax
from jax.experimental import pallas as pl
from jax.experimental.pallas import tpu as pltpu
from jax.sharding import Mesh
from jax.sharding import PartitionSpec as P


RESTART = 15
GY = ("gy_0", "gy_1", "gy_2")
ALL = ("gx",) + GY
FIELDS = 5
ROWS, COLS, LANES, HALO = 64, 256, 128, 32
FULL = 2 * ROWS
CENTRE, SPREAD, SHRINK = 5.8, 5.0, 0.9
SCALE = 2.0 * SHRINK / SPREAD
ALPHA = SCALE * CENTRE
SQUARE = SHRINK * SHRINK


def lane_group():
    return lax.broadcasted_iota(jnp.int32, (1, LANES), 1) // HALO


def packed_edges(tiles, lane):
    group = lane_group()
    top, bottom = None, None
    for q in range(4):
        shift = (HALO * q - lane) % LANES
        moved = pltpu.roll(tiles[q], shift, 1) if shift else tiles[q]
        part = tiles[4][16 * q : 16 * q + 16]
        part = pltpu.roll(part, shift, 1) if shift else part
        top = moved if q == 0 else jnp.where(group == q, moved, top)
        bottom = part if q == 0 else jnp.where(group == q, part, bottom)
    return top, bottom


def unpacked_edges(ref, base, lane):
    top = ref[base : base + ROWS, :]
    bottom = ref[base + ROWS : base + ROWS + 16, :]
    tiles, parts = [], []
    for q in range(4):
        shift = (lane - HALO * q) % LANES
        tiles.append(pltpu.roll(top, shift, 1) if shift else top)
        parts.append(pltpu.roll(bottom, shift, 1) if shift else bottom)
    return tiles + [jnp.concatenate(parts, axis=0)]


def pack_body(*refs):
    mine_at = lax.axis_index("gx")
    fields, (same_ref, cross_ref, partner_ref, held_ref) = refs[:FIELDS], refs[FIELDS:]
    for a in range(FIELDS):
        held_ref[a] = fields[a][...]

    def put(ref, base, edges):
        ref[base : base + ROWS, :] = edges[0]
        ref[base + ROWS : base + ROWS + 16, :] = edges[1]

    for core in (0, 1):

        @pl.when(mine_at == core)
        def _():
            left = [f[:, :LANES] for f in fields]
            right = [f[:, LANES:] for f in fields]
            give, keep = (right, left) if core == 0 else (left, right)
            for a in range(FIELDS):
                partner_ref[ROWS * a : ROWS * (a + 1), :] = give[a]
            put(partner_ref, FIELDS * ROWS, packed_edges(keep, 96 if core == 0 else 0))
            left_edge, right_edge = packed_edges(left, 0), packed_edges(right, 96)
            put(cross_ref, 0, left_edge if core == 0 else right_edge)
            put(same_ref, 0, right_edge if core == 0 else left_edge)


def basis_body(*refs):
    mine_at = lax.axis_index("gx")
    held_ref, partner_ref, cross_ref, same_ref, own_ref, give_ref, gram_ref = refs[:7]
    data, coef, basis, image, pairs = refs[7:]
    lane = lax.broadcasted_iota(jnp.int32, (1, LANES), 1)

    for core in (0, 1):

        @pl.when(mine_at == core)
        def _():
            mine, beside = (slice(0, LANES), slice(LANES, COLS))
            if core:
                mine, beside = beside, mine
            far = 96 if core == 0 else 0
            near = 96 - far
            same = unpacked_edges(same_ref, 0, far)
            cross = unpacked_edges(cross_ref, 0, far)
            inner = unpacked_edges(partner_ref, FIELDS * ROWS, near)
            for a in range(FIELDS):
                data[a, 8 : 8 + ROWS, :LANES] = held_ref[a, :, mine]
                data[a, 8 + ROWS : 8 + FULL, :LANES] = partner_ref[ROWS * a : ROWS * (a + 1), :]
                for row, here, there in ((8, held_ref[a, :, beside], same[a]), (8 + ROWS, inner[a], cross[a])):
                    low, high = (here, there) if core == 0 else (there, here)
                    tile = jnp.where(lane < HALO, low, jnp.where(lane >= LANES - HALO, high, 0.0))
                    data[a, row : row + ROWS, LANES:] = tile

    for a in range(FIELDS):
        data[a, 0:8, :] = data[a, FULL : FULL + 8, :]
        data[a, 8 + FULL : 16 + FULL, :] = data[a, 8:16, :]

    for r in range(0, FULL, 16):
        rows = slice(r, r + 16)
        at = lambda a, o: data[a, 8 + r + o : 24 + r + o, :]
        coef[0, rows, :] = SCALE * (at(2, 0) + (5.0 - CENTRE))
        vx, vy = at(3, 0), at(4, 0)
        for o in (1, 2):
            base = SCALE * (-4.0 / 3.0 if o == 1 else 1.0 / 12.0)
            turn = SCALE * (1.0 / 3.0 if o == 1 else -1.0 / 24.0)
            coef[4 * o - 3, rows, :] = base + turn * (vx + at(3, o))
            coef[4 * o - 2, rows, :] = base - turn * (vx + at(3, -o))
            coef[4 * o - 1, rows, :] = base + turn * (vy + pltpu.roll(vy, COLS - o, 1))
            coef[4 * o, rows, :] = base - turn * (vy + pltpu.roll(vy, o, 1))

    def stencil(load, r):
        rows = slice(r, r + 16)
        field = load(0)
        total = coef[0, rows, :] * field
        for o in (1, 2):
            total += coef[4 * o - 3, rows, :] * load(o)
            total += coef[4 * o - 2, rows, :] * load(-o)
            total += coef[4 * o - 1, rows, :] * pltpu.roll(field, COLS - o, 1)
            total += coef[4 * o, rows, :] * pltpu.roll(field, o, 1)
        return field, total

    def wrap(index):
        basis[index, 0:8, :] = basis[index, FULL : FULL + 8, :]
        basis[index, 8 + FULL : 16 + FULL, :] = basis[index, 8:16, :]

    basis[0, 8 : 8 + FULL, :] = jnp.zeros((FULL, COLS), jnp.float32)
    for r in range(0, FULL, 16):
        field, total = stencil(lambda o: data[1, 8 + r + o : 24 + r + o, :], r)
        start = data[0, 8 + r : 24 + r, :] - ((1.0 / SCALE) * total + CENTRE * field)
        basis[1, 8 + r : 24 + r, :] = start
        image[RESTART, r : r + 16, :] = start[:, :LANES]
    wrap(1)

    def step(j, carried):
        for r in range(0, FULL, 16):
            field, total = stencil(lambda o: basis[j + 1, 8 + r + o : 24 + r + o, :], r)
            image[j, r : r + 16, :] = total[:, :LANES] + ALPHA * field[:, :LANES]
            basis[j + 2, 8 + r : 24 + r, :] = total - SQUARE * basis[j, 8 + r : 24 + r, :]
        wrap(j + 2)
        return carried

    lax.fori_loop(0, RESTART, step, 0)
    own_ref[...] = basis[1:, 8 : 8 + ROWS, :LANES]
    give_ref[...] = basis[1:, 8 + ROWS : 8 + FULL, :LANES]

    for low in range(0, 16, 4):
        for high in range(low, 16, 4):

            def accumulate(t, sums):
                rows = pl.ds(pl.multiple_of(8 * t, 8), 8)
                first = [image[low + i, rows, :] for i in range(4)]
                second = first if low == high else [image[high + i, rows, :] for i in range(4)]
                return tuple(sums[4 * i + k] + first[i] * second[k] for i in range(4) for k in range(4))

            sums = lax.fori_loop(
                0, FULL // 8, accumulate, tuple(jnp.zeros((8, LANES), jnp.float32) for _ in range(16)), unroll=8
            )
            for i in range(4):
                for k in range(4):
                    row = jnp.sum(sums[4 * i + k], axis=0, keepdims=True)
                    at = 16 * (low + i) + high + k
                    pairs[at : at + 1, :] = row
                    if low != high:
                        at = 16 * (high + k) + low + i
                        pairs[at : at + 1, :] = row
    total = lax.dot_general(
        jnp.ones((8, LANES), jnp.float32),
        pairs[...],
        (((1,), (1,)), ((), ())),
        precision=lax.Precision.HIGHEST,
        preferred_element_type=jnp.float32,
    )
    both = jnp.concatenate([total[0:1, :LANES], total[0:1, LANES:]], axis=0)
    gram_ref[...] = jnp.broadcast_to(both[None], gram_ref.shape)


def finish_body(sums_ref, own_ref, got_ref, held_ref, solution_ref, residual_ref):
    total = jnp.sum(sums_ref[...], axis=0)
    total = jnp.concatenate([total[0:1], total[1:2]], axis=1)
    lane = lax.broadcasted_iota(jnp.int32, (16, COLS), 1)
    sub = lax.broadcasted_iota(jnp.int32, (16, COLS), 0)
    spread = jnp.where(lane // 16 == sub, total, 0.0)
    pick_row = lax.broadcasted_iota(jnp.int32, (COLS, LANES), 0) % 16
    pick_col = lax.broadcasted_iota(jnp.int32, (COLS, LANES), 1)
    pick = jnp.where(pick_row == pick_col, 1.0, 0.0)
    gram = jnp.dot(spread, pick, precision=lax.Precision.HIGHEST, preferred_element_type=jnp.float32)
    columns = [jnp.broadcast_to(gram[:, k : k + 1], (16, LANES)) for k in range(16)]
    row_at = lax.broadcasted_iota(jnp.int32, (16, LANES), 0)
    for k in range(RESTART):
        inverse = 1.0 / columns[k][k : k + 1, :]
        for j in range(k + 1, 16):
            top = columns[j][k : k + 1, :] * inverse
            columns[j] = jnp.where(row_at == k, top, columns[j] - columns[k] * top)
    z = [columns[RESTART][k : k + 1, :] for k in range(RESTART)]
    left = []
    for k in range(16):
        value = 1.0 if k == 0 else 0.0
        if k > 0:
            value = value - z[k - 1]
        if k < RESTART:
            value = value - ALPHA * z[k]
        if k + 1 < RESTART:
            value = value - SQUARE * z[k + 1]
        left.append(value)
    step = [SCALE * z[k] for k in range(RESTART)]
    first = lax.axis_index("gx") == 0
    for r in range(0, ROWS, 8):
        rows = slice(r, r + 8)
        sums = []
        for ref in (own_ref, got_ref):
            change, rest = None, None
            for k in range(16):
                vector = ref[k, rows, :]
                rest = left[k] * vector if k == 0 else rest + left[k] * vector
                if k < RESTART:
                    change = step[k] * vector if k == 0 else change + step[k] * vector
            sums.append((change, rest))
        (own_change, own_rest), (got_change, got_rest) = sums
        solution_ref[rows, :LANES] = held_ref[1, rows, :LANES] + jnp.where(first, own_change, got_change)
        solution_ref[rows, LANES:] = held_ref[1, rows, LANES:] + jnp.where(first, got_change, own_change)
        residual_ref[rows, :LANES] = jnp.where(first, own_rest, got_rest)
        residual_ref[rows, LANES:] = jnp.where(first, got_rest, own_rest)


def call(body, out_shape, scratch=(), staged=True):
    vmem = pl.BlockSpec(memory_space=pltpu.VMEM)

    def run(*args):
        if staged:
            args = [pltpu.with_memory_space_constraint(a, pltpu.VMEM) for a in args]
        return pl.pallas_call(
            body,
            out_shape=out_shape,
            in_specs=[vmem] * len(args),
            out_specs=tuple(vmem for _ in out_shape),
            scratch_shapes=scratch,
        )(*args)

    return run


def on_chip(*shape):
    return pltpu.VMEM(shape, jnp.float32)


def per_device(right_side, initial, reaction, velocity_x, velocity_y):
    fields = (right_side, initial, reaction, velocity_x, velocity_y)
    count = lax.axis_size(GY)
    swap = [(0, 1), (1, 0)]
    ahead = lambda g: (g + 1) % count
    behind = lambda g: (g - 1) % count
    cross = [(g, count + behind(g)) for g in range(count)] + [(count + g, ahead(g)) for g in range(count)]
    same = [(g, ahead(g)) for g in range(count)] + [(count + g, count + behind(g)) for g in range(count)]

    edge = on_chip(ROWS + 16, LANES)
    to_same, to_cross, to_partner, held = call(
        pack_body, (edge, edge, on_chip(FIELDS * ROWS + ROWS + 16, LANES), on_chip(FIELDS, ROWS, COLS)), staged=False
    )(*fields)
    from_same = lax.ppermute(to_same, ALL, same)
    from_cross = lax.ppermute(to_cross, ALL, cross)
    from_partner = lax.ppermute(to_partner, "gx", swap)
    own, give, gram = call(
        basis_body,
        (on_chip(16, ROWS, LANES), on_chip(16, ROWS, LANES), on_chip(2 * count, 2, LANES)),
        scratch=[
            on_chip(FIELDS, FULL + 16, COLS),
            on_chip(9, FULL, COLS),
            on_chip(RESTART + 2, FULL + 16, COLS),
            on_chip(16, FULL, LANES),
            on_chip(COLS, LANES),
        ],
    )(held, from_partner, from_cross, from_same)
    got = lax.ppermute(give, "gx", swap)
    sums = lax.all_to_all(gram, ALL, 0, 0, tiled=True)
    result = jax.ShapeDtypeStruct((ROWS, COLS), jnp.float32)
    return call(finish_body, (result, result))(sums, own, got, held)


def solution(mesh):
    torus = Mesh(mesh.devices.reshape(mesh.shape["gx"], 4, 4, 4), ALL)
    placed = P("gx", GY)
    return jax.shard_map(
        per_device,
        mesh=torus,
        in_specs=(placed,) * FIELDS,
        out_specs=(placed, placed),
        check_vma=False,
    )
```

```python
import jax
import jax.numpy as jnp
from jax import lax
from jax.experimental import pallas as pl
from jax.experimental.pallas import tpu as pltpu
from jax.sharding import Mesh
from jax.sharding import PartitionSpec as P


RESTART = 15
GY = ("gy_0", "gy_1", "gy_2")
ALL = ("gx",) + GY
FIELDS = 5
ROWS, COLS, LANES, HALO = 64, 256, 128, 32
FULL = 2 * ROWS
CENTRE, SPREAD, SHRINK = 5.8, 5.0, 0.9
SCALE = 2.0 * SHRINK / SPREAD
ALPHA = SCALE * CENTRE
SQUARE = SHRINK * SHRINK


def lane_group():
    return lax.broadcasted_iota(jnp.int32, (1, LANES), 1) // HALO


def packed_edges(tiles, lane):
    group = lane_group()
    top, bottom = None, None
    for q in range(4):
        shift = (HALO * q - lane) % LANES
        moved = pltpu.roll(tiles[q], shift, 1) if shift else tiles[q]
        part = tiles[4][16 * q : 16 * q + 16]
        part = pltpu.roll(part, shift, 1) if shift else part
        top = moved if q == 0 else jnp.where(group == q, moved, top)
        bottom = part if q == 0 else jnp.where(group == q, part, bottom)
    return top, bottom


def unpacked_edges(ref, base, lane):
    top = ref[base : base + ROWS, :]
    bottom = ref[base + ROWS : base + ROWS + 16, :]
    tiles, parts = [], []
    for q in range(4):
        shift = (lane - HALO * q) % LANES
        tiles.append(pltpu.roll(top, shift, 1) if shift else top)
        parts.append(pltpu.roll(bottom, shift, 1) if shift else bottom)
    return tiles + [jnp.concatenate(parts, axis=0)]


def pack_body(*refs):
    mine_at = lax.axis_index("gx")
    fields, (same_ref, cross_ref, partner_ref, held_ref) = refs[:FIELDS], refs[FIELDS:]
    for a in range(FIELDS):
        held_ref[a] = fields[a][...]

    def put(ref, base, edges):
        ref[base : base + ROWS, :] = edges[0]
        ref[base + ROWS : base + ROWS + 16, :] = edges[1]

    for core in (0, 1):

        @pl.when(mine_at == core)
        def _():
            left = [f[:, :LANES] for f in fields]
            right = [f[:, LANES:] for f in fields]
            give, keep = (right, left) if core == 0 else (left, right)
            for a in range(FIELDS):
                partner_ref[ROWS * a : ROWS * (a + 1), :] = give[a]
            put(partner_ref, FIELDS * ROWS, packed_edges(keep, 96 if core == 0 else 0))
            left_edge, right_edge = packed_edges(left, 0), packed_edges(right, 96)
            put(cross_ref, 0, left_edge if core == 0 else right_edge)
            put(same_ref, 0, right_edge if core == 0 else left_edge)


def basis_body(*refs):
    mine_at = lax.axis_index("gx")
    held_ref, partner_ref, cross_ref, same_ref, own_ref, give_ref, gram_ref = refs[:7]
    data, coef, basis, image, pairs = refs[7:]
    lane = lax.broadcasted_iota(jnp.int32, (1, LANES), 1)

    for core in (0, 1):

        @pl.when(mine_at == core)
        def _():
            mine, beside = (slice(0, LANES), slice(LANES, COLS))
            if core:
                mine, beside = beside, mine
            far = 96 if core == 0 else 0
            near = 96 - far
            same = unpacked_edges(same_ref, 0, far)
            cross = unpacked_edges(cross_ref, 0, far)
            inner = unpacked_edges(partner_ref, FIELDS * ROWS, near)
            for a in range(FIELDS):
                data[a, 0, 8 : 8 + ROWS, :] = held_ref[a, :, mine]
                data[a, 0, 8 + ROWS : 8 + FULL, :] = partner_ref[ROWS * a : ROWS * (a + 1), :]
                for row, here, there in ((8, held_ref[a, :, beside], same[a]), (8 + ROWS, inner[a], cross[a])):
                    low, high = (here, there) if core == 0 else (there, here)
                    tile = jnp.where(lane < HALO, low, jnp.where(lane >= LANES - HALO, high, 0.0))
                    data[a, 1, row : row + ROWS, :] = tile

    def turned(tiles, shift):
        one, two = (pltpu.roll(tile, shift % LANES, 1) for tile in tiles)
        over = lane < shift if shift > 0 else lane >= LANES + shift
        return jnp.where(over, two, one), jnp.where(over, one, two)

    def wrap(ref, index):
        for t in (0, 1):
            ref[index, t, 0:8, :] = ref[index, t, FULL : FULL + 8, :]
            ref[index, t, 8 + FULL : 16 + FULL, :] = ref[index, t, 8:16, :]

    def shifted(ref, index, r, o):
        return [ref[index, t, 8 + r + o : 24 + r + o, :] for t in (0, 1)]

    for a in range(FIELDS):
        wrap(data, a)

    for r in range(0, FULL, 16):
        rows = slice(r, r + 16)
        middle, vx, vy = (shifted(data, a, r, 0) for a in (2, 3, 4))
        for t in (0, 1):
            coef[0, t, rows, :] = SCALE * (middle[t] + (5.0 - CENTRE))
        for o in (1, 2):
            base = SCALE * (-4.0 / 3.0 if o == 1 else 1.0 / 12.0)
            turn = SCALE * (1.0 / 3.0 if o == 1 else -1.0 / 24.0)
            below, above = shifted(data, 3, r, o), shifted(data, 3, r, -o)
            ahead, behind = turned(vy, -o), turned(vy, o)
            for t in (0, 1):
                coef[4 * o - 3, t, rows, :] = base + turn * (vx[t] + below[t])
                coef[4 * o - 2, t, rows, :] = base - turn * (vx[t] + above[t])
                coef[4 * o - 1, t, rows, :] = base + turn * (vy[t] + ahead[t])
                coef[4 * o, t, rows, :] = base - turn * (vy[t] + behind[t])

    def stencil(ref, index, r):
        rows = slice(r, r + 16)
        field = shifted(ref, index, r, 0)
        total = [coef[0, t, rows, :] * field[t] for t in (0, 1)]
        for o in (1, 2):
            moved = (shifted(ref, index, r, o), shifted(ref, index, r, -o), turned(field, -o), turned(field, o))
            for k, tiles in enumerate(moved):
                total = [total[t] + coef[4 * o - 3 + k, t, rows, :] * tiles[t] for t in (0, 1)]
        return field, total

    for t in (0, 1):
        basis[0, t, 8 : 8 + FULL, :] = jnp.zeros((FULL, LANES), jnp.float32)
    for r in range(0, FULL, 16):
        field, total = stencil(data, 1, r)
        for t in (0, 1):
            start = data[0, t, 8 + r : 24 + r, :] - ((1.0 / SCALE) * total[t] + CENTRE * field[t])
            basis[1, t, 8 + r : 24 + r, :] = start
            if t == 0:
                image[RESTART, r : r + 16, :] = start
    wrap(basis, 1)

    def step(j, carried):
        for r in range(0, FULL, 16):
            field, total = stencil(basis, j + 1, r)
            image[j, r : r + 16, :] = total[0] + ALPHA * field[0]
            for t in (0, 1):
                basis[j + 2, t, 8 + r : 24 + r, :] = total[t] - SQUARE * basis[j, t, 8 + r : 24 + r, :]
        wrap(basis, j + 2)
        return carried

    lax.fori_loop(0, RESTART, step, 0)
    own_ref[...] = basis[1:, 0, 8 : 8 + ROWS, :]
    give_ref[...] = basis[1:, 0, 8 + ROWS : 8 + FULL, :]

    for low in range(0, 16, 4):
        for high in range(low, 16, 4):

            def accumulate(t, sums):
                rows = pl.ds(pl.multiple_of(8 * t, 8), 8)
                first = [image[low + i, rows, :] for i in range(4)]
                second = first if low == high else [image[high + i, rows, :] for i in range(4)]
                return tuple(sums[4 * i + k] + first[i] * second[k] for i in range(4) for k in range(4))

            sums = lax.fori_loop(
                0, FULL // 8, accumulate, tuple(jnp.zeros((8, LANES), jnp.float32) for _ in range(16)), unroll=8
            )
            for i in range(4):
                for k in range(4):
                    row = jnp.sum(sums[4 * i + k], axis=0, keepdims=True)
                    at = 16 * (low + i) + high + k
                    pairs[at : at + 1, :] = row
                    if low != high:
                        at = 16 * (high + k) + low + i
                        pairs[at : at + 1, :] = row
    total = lax.dot_general(
        jnp.ones((8, LANES), jnp.float32),
        pairs[...],
        (((1,), (1,)), ((), ())),
        precision=lax.Precision.HIGHEST,
        preferred_element_type=jnp.float32,
    )
    both = jnp.concatenate([total[0:1, :LANES], total[0:1, LANES:]], axis=0)
    gram_ref[...] = jnp.broadcast_to(both[None], gram_ref.shape)


def finish_body(sums_ref, own_ref, got_ref, held_ref, solution_ref, residual_ref):
    total = jnp.sum(sums_ref[...], axis=0)
    total = jnp.concatenate([total[0:1], total[1:2]], axis=1)
    lane = lax.broadcasted_iota(jnp.int32, (16, COLS), 1)
    sub = lax.broadcasted_iota(jnp.int32, (16, COLS), 0)
    spread = jnp.where(lane // 16 == sub, total, 0.0)
    pick_row = lax.broadcasted_iota(jnp.int32, (COLS, LANES), 0) % 16
    pick_col = lax.broadcasted_iota(jnp.int32, (COLS, LANES), 1)
    pick = jnp.where(pick_row == pick_col, 1.0, 0.0)
    gram = jnp.dot(spread, pick, precision=lax.Precision.HIGHEST, preferred_element_type=jnp.float32)
    columns = [jnp.broadcast_to(gram[:, k : k + 1], (16, LANES)) for k in range(16)]
    row_at = lax.broadcasted_iota(jnp.int32, (16, LANES), 0)
    for k in range(RESTART):
        inverse = 1.0 / columns[k][k : k + 1, :]
        for j in range(k + 1, 16):
            top = columns[j][k : k + 1, :] * inverse
            columns[j] = jnp.where(row_at == k, top, columns[j] - columns[k] * top)
    z = [columns[RESTART][k : k + 1, :] for k in range(RESTART)]
    left = []
    for k in range(16):
        value = 1.0 if k == 0 else 0.0
        if k > 0:
            value = value - z[k - 1]
        if k < RESTART:
            value = value - ALPHA * z[k]
        if k + 1 < RESTART:
            value = value - SQUARE * z[k + 1]
        left.append(value)
    step = [SCALE * z[k] for k in range(RESTART)]
    first = lax.axis_index("gx") == 0
    for r in range(0, ROWS, 8):
        rows = slice(r, r + 8)
        sums = []
        for ref in (own_ref, got_ref):
            change, rest = None, None
            for k in range(16):
                vector = ref[k, rows, :]
                rest = left[k] * vector if k == 0 else rest + left[k] * vector
                if k < RESTART:
                    change = step[k] * vector if k == 0 else change + step[k] * vector
            sums.append((change, rest))
        (own_change, own_rest), (got_change, got_rest) = sums
        solution_ref[rows, :LANES] = held_ref[1, rows, :LANES] + jnp.where(first, own_change, got_change)
        solution_ref[rows, LANES:] = held_ref[1, rows, LANES:] + jnp.where(first, got_change, own_change)
        residual_ref[rows, :LANES] = jnp.where(first, own_rest, got_rest)
        residual_ref[rows, LANES:] = jnp.where(first, got_rest, own_rest)


def call(body, out_shape, scratch=(), staged=True):
    vmem = pl.BlockSpec(memory_space=pltpu.VMEM)

    def run(*args):
        if staged:
            args = [pltpu.with_memory_space_constraint(a, pltpu.VMEM) for a in args]
        return pl.pallas_call(
            body,
            out_shape=out_shape,
            in_specs=[vmem] * len(args),
            out_specs=tuple(vmem for _ in out_shape),
            scratch_shapes=scratch,
        )(*args)

    return run


def on_chip(*shape):
    return pltpu.VMEM(shape, jnp.float32)


def per_device(right_side, initial, reaction, velocity_x, velocity_y):
    fields = (right_side, initial, reaction, velocity_x, velocity_y)
    count = lax.axis_size(GY)
    swap = [(0, 1), (1, 0)]
    ahead = lambda g: (g + 1) % count
    behind = lambda g: (g - 1) % count
    cross = [(g, count + behind(g)) for g in range(count)] + [(count + g, ahead(g)) for g in range(count)]
    same = [(g, ahead(g)) for g in range(count)] + [(count + g, count + behind(g)) for g in range(count)]

    edge = on_chip(ROWS + 16, LANES)
    to_same, to_cross, to_partner, held = call(
        pack_body, (edge, edge, on_chip(FIELDS * ROWS + ROWS + 16, LANES), on_chip(FIELDS, ROWS, COLS)), staged=False
    )(*fields)
    from_same = lax.ppermute(to_same, ALL, same)
    from_cross = lax.ppermute(to_cross, ALL, cross)
    from_partner = lax.ppermute(to_partner, "gx", swap)
    own, give, gram = call(
        basis_body,
        (on_chip(16, ROWS, LANES), on_chip(16, ROWS, LANES), on_chip(2 * count, 2, LANES)),
        scratch=[
            on_chip(FIELDS, 2, FULL + 16, LANES),
            on_chip(9, 2, FULL, LANES),
            on_chip(RESTART + 2, 2, FULL + 16, LANES),
            on_chip(16, FULL, LANES),
            on_chip(COLS, LANES),
        ],
    )(held, from_partner, from_cross, from_same)
    got = lax.ppermute(give, "gx", swap)
    sums = lax.all_to_all(gram, ALL, 0, 0, tiled=True)
    result = jax.ShapeDtypeStruct((ROWS, COLS), jnp.float32)
    return call(finish_body, (result, result))(sums, own, got, held)


def solution(mesh):
    torus = Mesh(mesh.devices.reshape(mesh.shape["gx"], 4, 4, 4), ALL)
    placed = P("gx", GY)
    return jax.shard_map(
        per_device,
        mesh=torus,
        in_specs=(placed,) * FIELDS,
        out_specs=(placed, placed),
        check_vma=False,
    )
```

```python
import jax
import jax.numpy as jnp
from jax import lax
from jax.experimental import pallas as pl
from jax.experimental.pallas import tpu as pltpu
from jax.sharding import Mesh
from jax.sharding import PartitionSpec as P


RESTART = 15
GY = ("gy_0", "gy_1", "gy_2")
ALL = ("gx",) + GY
FIELDS = 5
ROWS, COLS, LANES, HALO = 64, 256, 128, 32
FULL = 2 * ROWS
CENTRE, SPREAD, SHRINK = 5.8, 5.0, 0.9
SCALE = 2.0 * SHRINK / SPREAD
ALPHA = SCALE * CENTRE
SQUARE = SHRINK * SHRINK


def lane_group():
    return lax.broadcasted_iota(jnp.int32, (1, LANES), 1) // HALO


def packed_edges(tiles, lane):
    group = lane_group()
    top, bottom = None, None
    for q in range(4):
        shift = (HALO * q - lane) % LANES
        moved = pltpu.roll(tiles[q], shift, 1) if shift else tiles[q]
        part = tiles[4][16 * q : 16 * q + 16]
        part = pltpu.roll(part, shift, 1) if shift else part
        top = moved if q == 0 else jnp.where(group == q, moved, top)
        bottom = part if q == 0 else jnp.where(group == q, part, bottom)
    return top, bottom


def unpacked_edges(ref, base, lane):
    top = ref[base : base + ROWS, :]
    bottom = ref[base + ROWS : base + ROWS + 16, :]
    tiles, parts = [], []
    for q in range(4):
        shift = (lane - HALO * q) % LANES
        tiles.append(pltpu.roll(top, shift, 1) if shift else top)
        parts.append(pltpu.roll(bottom, shift, 1) if shift else bottom)
    return tiles + [jnp.concatenate(parts, axis=0)]


def pack_body(*refs):
    mine_at = lax.axis_index("gx")
    fields, (same_ref, cross_ref, partner_ref, held_ref) = refs[:FIELDS], refs[FIELDS:]
    for a in range(FIELDS):
        held_ref[a] = fields[a][...]

    def put(ref, base, edges):
        ref[base : base + ROWS, :] = edges[0]
        ref[base + ROWS : base + ROWS + 16, :] = edges[1]

    for core in (0, 1):

        @pl.when(mine_at == core)
        def _():
            left = [f[:, :LANES] for f in fields]
            right = [f[:, LANES:] for f in fields]
            give, keep = (right, left) if core == 0 else (left, right)
            for a in range(FIELDS):
                partner_ref[ROWS * a : ROWS * (a + 1), :] = give[a]
            put(partner_ref, FIELDS * ROWS, packed_edges(keep, 96 if core == 0 else 0))
            left_edge, right_edge = packed_edges(left, 0), packed_edges(right, 96)
            put(cross_ref, 0, left_edge if core == 0 else right_edge)
            put(same_ref, 0, right_edge if core == 0 else left_edge)


def basis_body(*refs):
    mine_at = lax.axis_index("gx")
    held_ref, partner_ref, cross_ref, same_ref, own_ref, give_ref, gram_ref = refs[:7]
    data, coef, image, pairs, *turns = refs[7:]
    lane = lax.broadcasted_iota(jnp.int32, (1, LANES), 1)

    for core in (0, 1):

        @pl.when(mine_at == core)
        def _():
            mine, beside = (slice(0, LANES), slice(LANES, COLS))
            if core:
                mine, beside = beside, mine
            far = 96 if core == 0 else 0
            near = 96 - far
            same = unpacked_edges(same_ref, 0, far)
            cross = unpacked_edges(cross_ref, 0, far)
            inner = unpacked_edges(partner_ref, FIELDS * ROWS, near)
            for a in range(FIELDS):
                data[a, 0, 8 : 8 + ROWS, :] = held_ref[a, :, mine]
                data[a, 0, 8 + ROWS : 8 + FULL, :] = partner_ref[ROWS * a : ROWS * (a + 1), :]
                for row, here, there in ((8, held_ref[a, :, beside], same[a]), (8 + ROWS, inner[a], cross[a])):
                    low, high = (here, there) if core == 0 else (there, here)
                    tile = jnp.where(lane < HALO, low, jnp.where(lane >= LANES - HALO, high, 0.0))
                    data[a, 1, row : row + ROWS, :] = tile

    def turned(tiles, shift):
        one, two = (pltpu.roll(tile, shift % LANES, 1) for tile in tiles)
        over = lane < shift if shift > 0 else lane >= LANES + shift
        return jnp.where(over, two, one), jnp.where(over, one, two)

    def wrap(ref, index):
        for t in (0, 1):
            ref[index, t, 0:8, :] = ref[index, t, FULL : FULL + 8, :]
            ref[index, t, 8 + FULL : 16 + FULL, :] = ref[index, t, 8:16, :]

    def shifted(ref, index, r, o):
        return [ref[index, t, 8 + r + o : 24 + r + o, :] for t in (0, 1)]

    for a in range(FIELDS):
        wrap(data, a)

    for r in range(0, FULL, 16):
        rows = slice(r, r + 16)
        middle, vx, vy = (shifted(data, a, r, 0) for a in (2, 3, 4))
        for t in (0, 1):
            coef[0, t, rows, :] = SCALE * (middle[t] + (5.0 - CENTRE))
        for o in (1, 2):
            base = SCALE * (-4.0 / 3.0 if o == 1 else 1.0 / 12.0)
            turn = SCALE * (1.0 / 3.0 if o == 1 else -1.0 / 24.0)
            below, above = shifted(data, 3, r, o), shifted(data, 3, r, -o)
            ahead, behind = turned(vy, -o), turned(vy, o)
            for t in (0, 1):
                coef[4 * o - 3, t, rows, :] = base + turn * (vx[t] + below[t])
                coef[4 * o - 2, t, rows, :] = base - turn * (vx[t] + above[t])
                coef[4 * o - 1, t, rows, :] = base + turn * (vy[t] + ahead[t])
                coef[4 * o, t, rows, :] = base - turn * (vy[t] + behind[t])

    def stencil(ref, index, r):
        rows = slice(r, r + 16)
        field = shifted(ref, index, r, 0)
        total = [coef[0, t, rows, :] * field[t] for t in (0, 1)]
        for o in (1, 2):
            moved = (shifted(ref, index, r, o), shifted(ref, index, r, -o), turned(field, -o), turned(field, o))
            for k, tiles in enumerate(moved):
                total = [total[t] + coef[4 * o - 3 + k, t, rows, :] * tiles[t] for t in (0, 1)]
        return field, total

    def keep(k, r, tile):
        if r < ROWS:
            own_ref[k, r : r + 16, :] = tile
        else:
            give_ref[k, r - ROWS : r - ROWS + 16, :] = tile

    for t in (0, 1):
        turns[0][0, t, 8 : 8 + FULL, :] = jnp.zeros((FULL, LANES), jnp.float32)
    for r in range(0, FULL, 16):
        field, total = stencil(data, 1, r)
        for t in (0, 1):
            start = data[0, t, 8 + r : 24 + r, :] - ((1.0 / SCALE) * total[t] + CENTRE * field[t])
            turns[1][0, t, 8 + r : 24 + r, :] = start
            if t == 0:
                image[RESTART, r : r + 16, :] = start
                keep(0, r, start)
    wrap(turns[1], 0)

    def steps(third, carried):
        for u in range(3):
            j = 3 * third + u
            past, now, later = turns[u], turns[(u + 1) % 3], turns[(u + 2) % 3]
            for r in range(0, FULL, 16):
                field, total = stencil(now, 0, r)
                image[j, r : r + 16, :] = total[0] + ALPHA * field[0]
                for t in (0, 1):
                    tile = total[t] - SQUARE * past[0, t, 8 + r : 24 + r, :]
                    later[0, t, 8 + r : 24 + r, :] = tile
                    if t == 0:
                        keep(j + 1, r, tile)
            wrap(later, 0)
        return carried

    lax.fori_loop(0, RESTART // 3, steps, 0)

    for low in range(0, 16, 4):
        for high in range(low, 16, 4):

            def accumulate(t, sums):
                rows = pl.ds(pl.multiple_of(8 * t, 8), 8)
                first = [image[low + i, rows, :] for i in range(4)]
                second = first if low == high else [image[high + i, rows, :] for i in range(4)]
                return tuple(sums[4 * i + k] + first[i] * second[k] for i in range(4) for k in range(4))

            sums = lax.fori_loop(
                0, FULL // 8, accumulate, tuple(jnp.zeros((8, LANES), jnp.float32) for _ in range(16)), unroll=8
            )
            for i in range(4):
                for k in range(4):
                    row = jnp.sum(sums[4 * i + k], axis=0, keepdims=True)
                    at = 16 * (low + i) + high + k
                    pairs[at : at + 1, :] = row
                    if low != high:
                        at = 16 * (high + k) + low + i
                        pairs[at : at + 1, :] = row
    total = lax.dot_general(
        jnp.ones((8, LANES), jnp.float32),
        pairs[...],
        (((1,), (1,)), ((), ())),
        precision=lax.Precision.HIGHEST,
        preferred_element_type=jnp.float32,
    )
    both = jnp.concatenate([total[0:1, :LANES], total[0:1, LANES:]], axis=0)
    gram_ref[...] = jnp.broadcast_to(both[None], gram_ref.shape)


def finish_body(sums_ref, own_ref, got_ref, held_ref, solution_ref, residual_ref):
    total = jnp.sum(sums_ref[...], axis=0)
    total = jnp.concatenate([total[0:1], total[1:2]], axis=1)
    lane = lax.broadcasted_iota(jnp.int32, (16, COLS), 1)
    sub = lax.broadcasted_iota(jnp.int32, (16, COLS), 0)
    spread = jnp.where(lane // 16 == sub, total, 0.0)
    pick_row = lax.broadcasted_iota(jnp.int32, (COLS, LANES), 0) % 16
    pick_col = lax.broadcasted_iota(jnp.int32, (COLS, LANES), 1)
    pick = jnp.where(pick_row == pick_col, 1.0, 0.0)
    gram = jnp.dot(spread, pick, precision=lax.Precision.HIGHEST, preferred_element_type=jnp.float32)
    columns = [jnp.broadcast_to(gram[:, k : k + 1], (16, LANES)) for k in range(16)]
    row_at = lax.broadcasted_iota(jnp.int32, (16, LANES), 0)
    for k in range(RESTART):
        inverse = 1.0 / columns[k][k : k + 1, :]
        for j in range(k + 1, 16):
            top = columns[j][k : k + 1, :] * inverse
            columns[j] = jnp.where(row_at == k, top, columns[j] - columns[k] * top)
    z = [columns[RESTART][k : k + 1, :] for k in range(RESTART)]
    left = []
    for k in range(16):
        value = 1.0 if k == 0 else 0.0
        if k > 0:
            value = value - z[k - 1]
        if k < RESTART:
            value = value - ALPHA * z[k]
        if k + 1 < RESTART:
            value = value - SQUARE * z[k + 1]
        left.append(value)
    step = [SCALE * z[k] for k in range(RESTART)]
    first = lax.axis_index("gx") == 0
    for r in range(0, ROWS, 8):
        rows = slice(r, r + 8)
        sums = []
        for ref in (own_ref, got_ref):
            change, rest = None, None
            for k in range(16):
                vector = ref[k, rows, :]
                rest = left[k] * vector if k == 0 else rest + left[k] * vector
                if k < RESTART:
                    change = step[k] * vector if k == 0 else change + step[k] * vector
            sums.append((change, rest))
        (own_change, own_rest), (got_change, got_rest) = sums
        solution_ref[rows, :LANES] = held_ref[1, rows, :LANES] + jnp.where(first, own_change, got_change)
        solution_ref[rows, LANES:] = held_ref[1, rows, LANES:] + jnp.where(first, got_change, own_change)
        residual_ref[rows, :LANES] = jnp.where(first, own_rest, got_rest)
        residual_ref[rows, LANES:] = jnp.where(first, got_rest, own_rest)


def call(body, out_shape, scratch=(), staged=True):
    vmem = pl.BlockSpec(memory_space=pltpu.VMEM)

    def run(*args):
        if staged:
            args = [pltpu.with_memory_space_constraint(a, pltpu.VMEM) for a in args]
        return pl.pallas_call(
            body,
            out_shape=out_shape,
            in_specs=[vmem] * len(args),
            out_specs=tuple(vmem for _ in out_shape),
            scratch_shapes=scratch,
        )(*args)

    return run


def on_chip(*shape):
    return pltpu.VMEM(shape, jnp.float32)


def per_device(right_side, initial, reaction, velocity_x, velocity_y):
    fields = (right_side, initial, reaction, velocity_x, velocity_y)
    count = lax.axis_size(GY)
    swap = [(0, 1), (1, 0)]
    ahead = lambda g: (g + 1) % count
    behind = lambda g: (g - 1) % count
    cross = [(g, count + behind(g)) for g in range(count)] + [(count + g, ahead(g)) for g in range(count)]
    same = [(g, ahead(g)) for g in range(count)] + [(count + g, count + behind(g)) for g in range(count)]

    edge = on_chip(ROWS + 16, LANES)
    to_same, to_cross, to_partner, held = call(
        pack_body, (edge, edge, on_chip(FIELDS * ROWS + ROWS + 16, LANES), on_chip(FIELDS, ROWS, COLS)), staged=False
    )(*fields)
    from_same = lax.ppermute(to_same, ALL, same)
    from_cross = lax.ppermute(to_cross, ALL, cross)
    from_partner = lax.ppermute(to_partner, "gx", swap)
    own, give, gram = call(
        basis_body,
        (on_chip(16, ROWS, LANES), on_chip(16, ROWS, LANES), on_chip(2 * count, 2, LANES)),
        scratch=[
            on_chip(FIELDS, 2, FULL + 16, LANES),
            on_chip(9, 2, FULL, LANES),
            on_chip(16, FULL, LANES),
            on_chip(COLS, LANES),
            *(on_chip(1, 2, FULL + 16, LANES) for _ in range(3)),
        ],
    )(held, from_partner, from_cross, from_same)
    got = lax.ppermute(give, "gx", swap)
    sums = lax.all_to_all(gram, ALL, 0, 0, tiled=True)
    result = jax.ShapeDtypeStruct((ROWS, COLS), jnp.float32)
    return call(finish_body, (result, result))(sums, own, got, held)


def solution(mesh):
    torus = Mesh(mesh.devices.reshape(mesh.shape["gx"], 4, 4, 4), ALL)
    placed = P("gx", GY)
    return jax.shard_map(
        per_device,
        mesh=torus,
        in_specs=(placed,) * FIELDS,
        out_specs=(placed, placed),
        check_vma=False,
    )
```

```python
import jax
import jax.numpy as jnp
from jax import lax
from jax.experimental import pallas as pl
from jax.experimental.pallas import tpu as pltpu
from jax.sharding import Mesh
from jax.sharding import PartitionSpec as P


RESTART = 15
GY = ("gy_0", "gy_1", "gy_2")
ALL = ("gx",) + GY
FIELDS = 5
ROWS, COLS, LANES, HALO = 64, 256, 128, 32
FULL = 2 * ROWS
CENTRE, SPREAD, SHRINK = 5.8, 5.0, 0.9
SCALE = 2.0 * SHRINK / SPREAD
ALPHA = SCALE * CENTRE
SQUARE = SHRINK * SHRINK


def lane_group():
    return lax.broadcasted_iota(jnp.int32, (1, LANES), 1) // HALO


def packed_edges(tiles, lane):
    group = lane_group()
    top, bottom = None, None
    for q in range(4):
        shift = (HALO * q - lane) % LANES
        moved = pltpu.roll(tiles[q], shift, 1) if shift else tiles[q]
        part = tiles[4][16 * q : 16 * q + 16]
        part = pltpu.roll(part, shift, 1) if shift else part
        top = moved if q == 0 else jnp.where(group == q, moved, top)
        bottom = part if q == 0 else jnp.where(group == q, part, bottom)
    return top, bottom


def unpacked_edges(ref, base, lane):
    top = ref[base : base + ROWS, :]
    bottom = ref[base + ROWS : base + ROWS + 16, :]
    tiles, parts = [], []
    for q in range(4):
        shift = (lane - HALO * q) % LANES
        tiles.append(pltpu.roll(top, shift, 1) if shift else top)
        parts.append(pltpu.roll(bottom, shift, 1) if shift else bottom)
    return tiles + [jnp.concatenate(parts, axis=0)]


def pack_body(*refs):
    mine_at = lax.axis_index("gx")
    fields, (same_ref, cross_ref, partner_ref, held_ref) = refs[:FIELDS], refs[FIELDS:]
    for a in range(FIELDS):
        held_ref[a] = fields[a][...]

    def put(ref, base, edges):
        ref[base : base + ROWS, :] = edges[0]
        ref[base + ROWS : base + ROWS + 16, :] = edges[1]

    for core in (0, 1):

        @pl.when(mine_at == core)
        def _():
            left = [f[:, :LANES] for f in fields]
            right = [f[:, LANES:] for f in fields]
            give, keep = (right, left) if core == 0 else (left, right)
            for a in range(FIELDS):
                partner_ref[ROWS * a : ROWS * (a + 1), :] = give[a]
            put(partner_ref, FIELDS * ROWS, packed_edges(keep, 96 if core == 0 else 0))
            left_edge, right_edge = packed_edges(left, 0), packed_edges(right, 96)
            put(cross_ref, 0, left_edge if core == 0 else right_edge)
            put(same_ref, 0, right_edge if core == 0 else left_edge)


def basis_body(*refs):
    mine_at = lax.axis_index("gx")
    held_ref, partner_ref, cross_ref, same_ref, own_ref, give_ref, gram_ref = refs[:7]
    data, coef, image, pairs, *turns = refs[7:]
    lane = lax.broadcasted_iota(jnp.int32, (1, LANES), 1)

    for core in (0, 1):

        @pl.when(mine_at == core)
        def _():
            mine, beside = (slice(0, LANES), slice(LANES, COLS))
            if core:
                mine, beside = beside, mine
            far = 96 if core == 0 else 0
            near = 96 - far
            same = unpacked_edges(same_ref, 0, far)
            cross = unpacked_edges(cross_ref, 0, far)
            inner = unpacked_edges(partner_ref, FIELDS * ROWS, near)
            for a in range(FIELDS):
                data[a, 0, 8 : 8 + ROWS, :] = held_ref[a, :, mine]
                data[a, 0, 8 + ROWS : 8 + FULL, :] = partner_ref[ROWS * a : ROWS * (a + 1), :]
                for row, here, there in ((8, held_ref[a, :, beside], same[a]), (8 + ROWS, inner[a], cross[a])):
                    low, high = (here, there) if core == 0 else (there, here)
                    tile = jnp.where(lane < HALO, low, jnp.where(lane >= LANES - HALO, high, 0.0))
                    data[a, 1, row : row + ROWS, :] = tile

    def turned(tiles, shift):
        one, two = (pltpu.roll(tile, shift % LANES, 1) for tile in tiles)
        over = lane < shift if shift > 0 else lane >= LANES + shift
        return jnp.where(over, two, one), jnp.where(over, one, two)

    def wrap(ref, index):
        for t in (0, 1):
            ref[index, t, 0:8, :] = ref[index, t, FULL : FULL + 8, :]
            ref[index, t, 8 + FULL : 16 + FULL, :] = ref[index, t, 8:16, :]

    def shifted(ref, index, r, o):
        return [ref[index, t, 8 + r + o : 24 + r + o, :] for t in (0, 1)]

    for a in range(FIELDS):
        wrap(data, a)

    for r in range(0, FULL, 16):
        rows = slice(r, r + 16)
        middle, vx, vy = (shifted(data, a, r, 0) for a in (2, 3, 4))
        for t in (0, 1):
            coef[0, t, rows, :] = SCALE * (middle[t] + (5.0 - CENTRE))
        for o in (1, 2):
            base = SCALE * (-4.0 / 3.0 if o == 1 else 1.0 / 12.0)
            turn = SCALE * (1.0 / 3.0 if o == 1 else -1.0 / 24.0)
            below, above = shifted(data, 3, r, o), shifted(data, 3, r, -o)
            ahead, behind = turned(vy, -o), turned(vy, o)
            for t in (0, 1):
                coef[4 * o - 3, t, rows, :] = base + turn * (vx[t] + below[t])
                coef[4 * o - 2, t, rows, :] = base - turn * (vx[t] + above[t])
                coef[4 * o - 1, t, rows, :] = base + turn * (vy[t] + ahead[t])
                coef[4 * o, t, rows, :] = base - turn * (vy[t] + behind[t])

    def stencil(ref, index, r):
        rows = slice(r, r + 16)
        field = shifted(ref, index, r, 0)
        total = [coef[0, t, rows, :] * field[t] for t in (0, 1)]
        for o in (1, 2):
            moved = (shifted(ref, index, r, o), shifted(ref, index, r, -o), turned(field, -o), turned(field, o))
            for k, tiles in enumerate(moved):
                total = [total[t] + coef[4 * o - 3 + k, t, rows, :] * tiles[t] for t in (0, 1)]
        return field, total

    def keep(k, r, tile):
        if r < ROWS:
            own_ref[k, r : r + 16, :] = tile
        else:
            give_ref[k, r - ROWS : r - ROWS + 16, :] = tile

    for t in (0, 1):
        turns[0][0, t, 8 : 8 + FULL, :] = jnp.zeros((FULL, LANES), jnp.float32)
    for r in range(0, FULL, 16):
        field, total = stencil(data, 1, r)
        for t in (0, 1):
            start = data[0, t, 8 + r : 24 + r, :] - ((1.0 / SCALE) * total[t] + CENTRE * field[t])
            turns[1][0, t, 8 + r : 24 + r, :] = start
            if t == 0:
                image[RESTART, r : r + 16, :] = start
                keep(0, r, start)
    wrap(turns[1], 0)

    def steps(third, carried):
        for u in range(3):
            j = 3 * third + u
            past, now, later = turns[u], turns[(u + 1) % 3], turns[(u + 2) % 3]
            for r in range(0, FULL, 16):
                field, total = stencil(now, 0, r)
                image[j, r : r + 16, :] = total[0] + ALPHA * field[0]
                for t in (0, 1):
                    tile = total[t] - SQUARE * past[0, t, 8 + r : 24 + r, :]
                    later[0, t, 8 + r : 24 + r, :] = tile
                    if t == 0:
                        keep(j + 1, r, tile)
            wrap(later, 0)
        return carried

    lax.fori_loop(0, RESTART // 3, steps, 0)

    for low in range(0, 16, 4):
        for high in range(low, 16, 4):
            wanted = [(i, k) for i in range(4) for k in range(4) if low != high or i <= k]

            def accumulate(t, sums):
                rows = pl.ds(pl.multiple_of(8 * t, 8), 8)
                first = [image[low + i, rows, :] for i in range(4)]
                second = first if low == high else [image[high + i, rows, :] for i in range(4)]
                return tuple(total + first[i] * second[k] for total, (i, k) in zip(sums, wanted))

            zeros = tuple(jnp.zeros((8, LANES), jnp.float32) for _ in wanted)
            sums = lax.fori_loop(0, FULL // 8, accumulate, zeros, unroll=16)
            for total, (i, k) in zip(sums, wanted):
                row = jnp.sum(total, axis=0, keepdims=True)
                for at in sorted({16 * (low + i) + high + k, 16 * (high + k) + low + i}):
                    pairs[at : at + 1, :] = row
    total = lax.dot_general(
        jnp.ones((8, LANES), jnp.float32),
        pairs[...],
        (((1,), (1,)), ((), ())),
        precision=lax.Precision.HIGHEST,
        preferred_element_type=jnp.float32,
    )
    both = jnp.concatenate([total[0:1, :LANES], total[0:1, LANES:]], axis=0)
    gram_ref[...] = jnp.broadcast_to(both[None], gram_ref.shape)


def finish_body(sums_ref, own_ref, got_ref, held_ref, solution_ref, residual_ref):
    total = jnp.sum(jnp.sum(sums_ref[...].reshape(-1, 8, 2, LANES), axis=0), axis=0)
    total = jnp.concatenate([total[0:1], total[1:2]], axis=1)
    lane = lax.broadcasted_iota(jnp.int32, (16, COLS), 1)
    sub = lax.broadcasted_iota(jnp.int32, (16, COLS), 0)
    spread = jnp.where(lane // 16 == sub, total, 0.0)
    pick_row = lax.broadcasted_iota(jnp.int32, (COLS, LANES), 0) % 16
    pick_col = lax.broadcasted_iota(jnp.int32, (COLS, LANES), 1)
    pick = jnp.where(pick_row == pick_col, 1.0, 0.0)
    gram = jnp.dot(spread, pick, precision=lax.Precision.HIGHEST, preferred_element_type=jnp.float32)
    columns = [jnp.broadcast_to(gram[:, k : k + 1], (16, LANES)) for k in range(16)]
    row_at = lax.broadcasted_iota(jnp.int32, (16, LANES), 0)
    for k in range(RESTART):
        inverse = 1.0 / columns[k][k : k + 1, :]
        for j in range(k + 1, 16):
            top = columns[j][k : k + 1, :] * inverse
            columns[j] = jnp.where(row_at == k, top, columns[j] - columns[k] * top)
    z = [columns[RESTART][k : k + 1, :] for k in range(RESTART)]
    left = []
    for k in range(16):
        value = 1.0 if k == 0 else 0.0
        if k > 0:
            value = value - z[k - 1]
        if k < RESTART:
            value = value - ALPHA * z[k]
        if k + 1 < RESTART:
            value = value - SQUARE * z[k + 1]
        left.append(value)
    step = [SCALE * z[k] for k in range(RESTART)]
    first = lax.axis_index("gx") == 0
    for r in range(0, ROWS, 8):
        rows = slice(r, r + 8)
        sums = []
        for ref in (own_ref, got_ref):
            change, rest = None, None
            for k in range(16):
                vector = ref[k, rows, :]
                rest = left[k] * vector if k == 0 else rest + left[k] * vector
                if k < RESTART:
                    change = step[k] * vector if k == 0 else change + step[k] * vector
            sums.append((change, rest))
        (own_change, own_rest), (got_change, got_rest) = sums
        solution_ref[rows, :LANES] = held_ref[1, rows, :LANES] + jnp.where(first, own_change, got_change)
        solution_ref[rows, LANES:] = held_ref[1, rows, LANES:] + jnp.where(first, got_change, own_change)
        residual_ref[rows, :LANES] = jnp.where(first, own_rest, got_rest)
        residual_ref[rows, LANES:] = jnp.where(first, got_rest, own_rest)


def call(body, out_shape, scratch=(), staged=True):
    vmem = pl.BlockSpec(memory_space=pltpu.VMEM)

    def run(*args):
        if staged:
            args = [pltpu.with_memory_space_constraint(a, pltpu.VMEM) for a in args]
        return pl.pallas_call(
            body,
            out_shape=out_shape,
            in_specs=[vmem] * len(args),
            out_specs=tuple(vmem for _ in out_shape),
            scratch_shapes=scratch,
        )(*args)

    return run


def on_chip(*shape):
    return pltpu.VMEM(shape, jnp.float32)


def per_device(right_side, initial, reaction, velocity_x, velocity_y):
    fields = (right_side, initial, reaction, velocity_x, velocity_y)
    count = lax.axis_size(GY)
    swap = [(0, 1), (1, 0)]
    ahead = lambda g: (g + 1) % count
    behind = lambda g: (g - 1) % count
    cross = [(g, count + behind(g)) for g in range(count)] + [(count + g, ahead(g)) for g in range(count)]
    same = [(g, ahead(g)) for g in range(count)] + [(count + g, count + behind(g)) for g in range(count)]

    edge = on_chip(ROWS + 16, LANES)
    to_same, to_cross, to_partner, held = call(
        pack_body, (edge, edge, on_chip(FIELDS * ROWS + ROWS + 16, LANES), on_chip(FIELDS, ROWS, COLS)), staged=False
    )(*fields)
    from_same = lax.ppermute(to_same, ALL, same)
    from_cross = lax.ppermute(to_cross, ALL, cross)
    from_partner = lax.ppermute(to_partner, "gx", swap)
    own, give, gram = call(
        basis_body,
        (on_chip(16, ROWS, LANES), on_chip(16, ROWS, LANES), on_chip(2 * count, 2, LANES)),
        scratch=[
            on_chip(FIELDS, 2, FULL + 16, LANES),
            on_chip(9, 2, FULL, LANES),
            on_chip(16, FULL, LANES),
            on_chip(COLS, LANES),
            *(on_chip(1, 2, FULL + 16, LANES) for _ in range(3)),
        ],
    )(held, from_partner, from_cross, from_same)
    got = lax.ppermute(give, "gx", swap)
    sums = lax.all_to_all(gram, ALL, 0, 0, tiled=True)
    result = jax.ShapeDtypeStruct((ROWS, COLS), jnp.float32)
    return call(finish_body, (result, result))(sums, own, got, held)


def solution(mesh):
    torus = Mesh(mesh.devices.reshape(mesh.shape["gx"], 4, 4, 4), ALL)
    placed = P("gx", GY)
    return jax.shard_map(
        per_device,
        mesh=torus,
        in_specs=(placed,) * FIELDS,
        out_specs=(placed, placed),
        check_vma=False,
    )
```

```python
import jax
import jax.numpy as jnp
from jax import lax
from jax.experimental import pallas as pl
from jax.experimental.pallas import tpu as pltpu
from jax.sharding import Mesh
from jax.sharding import PartitionSpec as P


RESTART = 15
GY = ("gy_0", "gy_1", "gy_2")
ALL = ("gx",) + GY
FIELDS = 5
ROWS, COLS, LANES, HALO = 64, 256, 128, 32
FULL = 2 * ROWS
CENTRE, SPREAD, SHRINK = 5.8, 5.0, 0.9
SCALE = 2.0 * SHRINK / SPREAD
ALPHA = SCALE * CENTRE
SQUARE = SHRINK * SHRINK


def lane_group():
    return lax.broadcasted_iota(jnp.int32, (1, LANES), 1) // HALO


def packed_edges(tiles, lane):
    group = lane_group()
    top, bottom = None, None
    for q in range(4):
        shift = (HALO * q - lane) % LANES
        moved = pltpu.roll(tiles[q], shift, 1) if shift else tiles[q]
        part = tiles[4][16 * q : 16 * q + 16]
        part = pltpu.roll(part, shift, 1) if shift else part
        top = moved if q == 0 else jnp.where(group == q, moved, top)
        bottom = part if q == 0 else jnp.where(group == q, part, bottom)
    return top, bottom


def unpacked_edges(ref, base, lane):
    top = ref[base : base + ROWS, :]
    bottom = ref[base + ROWS : base + ROWS + 16, :]
    tiles, parts = [], []
    for q in range(4):
        shift = (lane - HALO * q) % LANES
        tiles.append(pltpu.roll(top, shift, 1) if shift else top)
        parts.append(pltpu.roll(bottom, shift, 1) if shift else bottom)
    return tiles + [jnp.concatenate(parts, axis=0)]


def pack_body(*refs):
    mine_at = lax.axis_index("gx")
    fields, (same_ref, cross_ref, partner_ref, held_ref) = refs[:FIELDS], refs[FIELDS:]
    for a in range(FIELDS):
        held_ref[a] = fields[a][...]

    def put(ref, base, edges):
        ref[base : base + ROWS, :] = edges[0]
        ref[base + ROWS : base + ROWS + 16, :] = edges[1]

    for core in (0, 1):

        @pl.when(mine_at == core)
        def _():
            left = [f[:, :LANES] for f in fields]
            right = [f[:, LANES:] for f in fields]
            give, keep = (right, left) if core == 0 else (left, right)
            for a in range(FIELDS):
                partner_ref[ROWS * a : ROWS * (a + 1), :] = give[a]
            put(partner_ref, FIELDS * ROWS, packed_edges(keep, 96 if core == 0 else 0))
            left_edge, right_edge = packed_edges(left, 0), packed_edges(right, 96)
            put(cross_ref, 0, left_edge if core == 0 else right_edge)
            put(same_ref, 0, right_edge if core == 0 else left_edge)


def basis_body(*refs):
    mine_at = lax.axis_index("gx")
    held_ref, partner_ref, cross_ref, same_ref, own_ref, give_ref, gram_ref = refs[:7]
    data, coef, image, pairs, *turns = refs[7:]
    lane = lax.broadcasted_iota(jnp.int32, (1, LANES), 1)

    for core in (0, 1):

        @pl.when(mine_at == core)
        def _():
            mine, beside = (slice(0, LANES), slice(LANES, COLS))
            if core:
                mine, beside = beside, mine
            far = 96 if core == 0 else 0
            near = 96 - far
            same = unpacked_edges(same_ref, 0, far)
            cross = unpacked_edges(cross_ref, 0, far)
            inner = unpacked_edges(partner_ref, FIELDS * ROWS, near)
            for a in range(FIELDS):
                data[a, 0, 8 : 8 + ROWS, :] = held_ref[a, :, mine]
                data[a, 0, 8 + ROWS : 8 + FULL, :] = partner_ref[ROWS * a : ROWS * (a + 1), :]
                for row, here, there in ((8, held_ref[a, :, beside], same[a]), (8 + ROWS, inner[a], cross[a])):
                    low, high = (here, there) if core == 0 else (there, here)
                    tile = jnp.where(lane < HALO, low, jnp.where(lane >= LANES - HALO, high, 0.0))
                    data[a, 1, row : row + ROWS, :] = tile

    def turned(tiles, shift):
        one, two = (pltpu.roll(tile, shift % LANES, 1) for tile in tiles)
        over = lane < shift if shift > 0 else lane >= LANES + shift
        return jnp.where(over, two, one), jnp.where(over, one, two)

    def wrap(ref, index):
        for t in (0, 1):
            ref[index, t, 0:8, :] = ref[index, t, FULL : FULL + 8, :]
            ref[index, t, 8 + FULL : 16 + FULL, :] = ref[index, t, 8:16, :]

    def shifted(ref, index, r, o):
        return [ref[index, t, 8 + r + o : 24 + r + o, :] for t in (0, 1)]

    for a in range(FIELDS):
        wrap(data, a)

    for r in range(0, FULL, 16):
        rows = slice(r, r + 16)
        middle, vx, vy = (shifted(data, a, r, 0) for a in (2, 3, 4))
        for t in (0, 1):
            coef[0, t, rows, :] = SCALE * (middle[t] + (5.0 - CENTRE))
        for o in (1, 2):
            base = SCALE * (-4.0 / 3.0 if o == 1 else 1.0 / 12.0)
            turn = SCALE * (1.0 / 3.0 if o == 1 else -1.0 / 24.0)
            below, above = shifted(data, 3, r, o), shifted(data, 3, r, -o)
            ahead, behind = turned(vy, -o), turned(vy, o)
            for t in (0, 1):
                coef[4 * o - 3, t, rows, :] = base + turn * (vx[t] + below[t])
                coef[4 * o - 2, t, rows, :] = base - turn * (vx[t] + above[t])
                coef[4 * o - 1, t, rows, :] = base + turn * (vy[t] + ahead[t])
                coef[4 * o, t, rows, :] = base - turn * (vy[t] + behind[t])

    def stencil(ref, index, r):
        rows = slice(r, r + 16)
        field = shifted(ref, index, r, 0)
        total = [coef[0, t, rows, :] * field[t] for t in (0, 1)]
        for o in (1, 2):
            moved = (shifted(ref, index, r, o), shifted(ref, index, r, -o), turned(field, -o), turned(field, o))
            for k, tiles in enumerate(moved):
                total = [total[t] + coef[4 * o - 3 + k, t, rows, :] * tiles[t] for t in (0, 1)]
        return field, total

    def keep(k, r, tile):
        if r < ROWS:
            own_ref[k, r : r + 16, :] = tile
        else:
            give_ref[k, r - ROWS : r - ROWS + 16, :] = tile

    for t in (0, 1):
        turns[0][0, t, 8 : 8 + FULL, :] = jnp.zeros((FULL, LANES), jnp.float32)
    for r in range(0, FULL, 16):
        field, total = stencil(data, 1, r)
        for t in (0, 1):
            start = data[0, t, 8 + r : 24 + r, :] - ((1.0 / SCALE) * total[t] + CENTRE * field[t])
            turns[1][0, t, 8 + r : 24 + r, :] = start
            if t == 0:
                image[RESTART, r : r + 16, :] = start
                keep(0, r, start)
    wrap(turns[1], 0)

    def steps(third, carried):
        for u in range(3):
            j = 3 * third + u
            past, now, later = turns[u], turns[(u + 1) % 3], turns[(u + 2) % 3]
            for r in range(0, FULL, 16):
                field, total = stencil(now, 0, r)
                image[j, r : r + 16, :] = total[0] + ALPHA * field[0]
                for t in (0, 1):
                    tile = total[t] - SQUARE * past[0, t, 8 + r : 24 + r, :]
                    later[0, t, 8 + r : 24 + r, :] = tile
                    if t == 0:
                        keep(j + 1, r, tile)
            wrap(later, 0)
        return carried

    lax.fori_loop(0, RESTART // 3, steps, 0, unroll=RESTART // 3)

    for low in range(0, 16, 4):
        for high in range(low, 16, 4):

            def accumulate(t, sums):
                rows = pl.ds(pl.multiple_of(8 * t, 8), 8)
                first = [image[low + i, rows, :] for i in range(4)]
                second = first if low == high else [image[high + i, rows, :] for i in range(4)]
                return tuple(sums[4 * i + k] + first[i] * second[k] for i in range(4) for k in range(4))

            sums = lax.fori_loop(
                0, FULL // 8, accumulate, tuple(jnp.zeros((8, LANES), jnp.float32) for _ in range(16)), unroll=16
            )
            for i in range(4):
                for k in range(4):
                    row = jnp.sum(sums[4 * i + k], axis=0, keepdims=True)
                    at = 16 * (low + i) + high + k
                    pairs[at : at + 1, :] = row
                    if low != high:
                        at = 16 * (high + k) + low + i
                        pairs[at : at + 1, :] = row
    total = lax.dot_general(
        jnp.ones((8, LANES), jnp.float32),
        pairs[...],
        (((1,), (1,)), ((), ())),
        precision=lax.Precision.HIGHEST,
        preferred_element_type=jnp.float32,
    )
    both = jnp.concatenate([total[0:1, :LANES], total[0:1, LANES:]], axis=0)
    gram_ref[...] = jnp.broadcast_to(both[None], gram_ref.shape)


def finish_body(sums_ref, own_ref, got_ref, held_ref, solution_ref, residual_ref):
    total = jnp.sum(jnp.sum(sums_ref[...].reshape(-1, 8, 2, LANES), axis=0), axis=0)
    total = jnp.concatenate([total[0:1], total[1:2]], axis=1)
    lane = lax.broadcasted_iota(jnp.int32, (16, COLS), 1)
    sub = lax.broadcasted_iota(jnp.int32, (16, COLS), 0)
    spread = jnp.where(lane // 16 == sub, total, 0.0)
    pick_row = lax.broadcasted_iota(jnp.int32, (COLS, LANES), 0) % 16
    pick_col = lax.broadcasted_iota(jnp.int32, (COLS, LANES), 1)
    pick = jnp.where(pick_row == pick_col, 1.0, 0.0)
    gram = jnp.dot(spread, pick, precision=lax.Precision.HIGHEST, preferred_element_type=jnp.float32)
    columns = [jnp.broadcast_to(gram[:, k : k + 1], (16, LANES)) for k in range(16)]
    row_at = lax.broadcasted_iota(jnp.int32, (16, LANES), 0)
    for k in range(RESTART):
        inverse = 1.0 / columns[k][k : k + 1, :]
        for j in range(k + 1, 16):
            top = columns[j][k : k + 1, :] * inverse
            columns[j] = jnp.where(row_at == k, top, columns[j] - columns[k] * top)
    z = [columns[RESTART][k : k + 1, :] for k in range(RESTART)]
    left = []
    for k in range(16):
        value = 1.0 if k == 0 else 0.0
        if k > 0:
            value = value - z[k - 1]
        if k < RESTART:
            value = value - ALPHA * z[k]
        if k + 1 < RESTART:
            value = value - SQUARE * z[k + 1]
        left.append(value)
    step = [SCALE * z[k] for k in range(RESTART)]
    first = lax.axis_index("gx") == 0
    for r in range(0, ROWS, 8):
        rows = slice(r, r + 8)
        sums = []
        for ref in (own_ref, got_ref):
            change, rest = None, None
            for k in range(16):
                vector = ref[k, rows, :]
                rest = left[k] * vector if k == 0 else rest + left[k] * vector
                if k < RESTART:
                    change = step[k] * vector if k == 0 else change + step[k] * vector
            sums.append((change, rest))
        (own_change, own_rest), (got_change, got_rest) = sums
        solution_ref[rows, :LANES] = held_ref[1, rows, :LANES] + jnp.where(first, own_change, got_change)
        solution_ref[rows, LANES:] = held_ref[1, rows, LANES:] + jnp.where(first, got_change, own_change)
        residual_ref[rows, :LANES] = jnp.where(first, own_rest, got_rest)
        residual_ref[rows, LANES:] = jnp.where(first, got_rest, own_rest)


def call(body, out_shape, scratch=(), staged=True):
    vmem = pl.BlockSpec(memory_space=pltpu.VMEM)

    def run(*args):
        if staged:
            args = [pltpu.with_memory_space_constraint(a, pltpu.VMEM) for a in args]
        return pl.pallas_call(
            body,
            out_shape=out_shape,
            in_specs=[vmem] * len(args),
            out_specs=tuple(vmem for _ in out_shape),
            scratch_shapes=scratch,
        )(*args)

    return run


def on_chip(*shape):
    return pltpu.VMEM(shape, jnp.float32)


def per_device(right_side, initial, reaction, velocity_x, velocity_y):
    fields = (right_side, initial, reaction, velocity_x, velocity_y)
    count = lax.axis_size(GY)
    swap = [(0, 1), (1, 0)]
    ahead = lambda g: (g + 1) % count
    behind = lambda g: (g - 1) % count
    cross = [(g, count + behind(g)) for g in range(count)] + [(count + g, ahead(g)) for g in range(count)]
    same = [(g, ahead(g)) for g in range(count)] + [(count + g, count + behind(g)) for g in range(count)]

    edge = on_chip(ROWS + 16, LANES)
    to_same, to_cross, to_partner, held = call(
        pack_body, (edge, edge, on_chip(FIELDS * ROWS + ROWS + 16, LANES), on_chip(FIELDS, ROWS, COLS)), staged=False
    )(*fields)
    from_same = lax.ppermute(to_same, ALL, same)
    from_cross = lax.ppermute(to_cross, ALL, cross)
    from_partner = lax.ppermute(to_partner, "gx", swap)
    own, give, gram = call(
        basis_body,
        (on_chip(16, ROWS, LANES), on_chip(16, ROWS, LANES), on_chip(2 * count, 2, LANES)),
        scratch=[
            on_chip(FIELDS, 2, FULL + 16, LANES),
            on_chip(9, 2, FULL, LANES),
            on_chip(16, FULL, LANES),
            on_chip(COLS, LANES),
            *(on_chip(1, 2, FULL + 16, LANES) for _ in range(3)),
        ],
    )(held, from_partner, from_cross, from_same)
    got = lax.ppermute(give, "gx", swap)
    sums = lax.all_to_all(gram, ALL, 0, 0, tiled=True)
    result = jax.ShapeDtypeStruct((ROWS, COLS), jnp.float32)
    return call(finish_body, (result, result))(sums, own, got, held)


def solution(mesh):
    torus = Mesh(mesh.devices.reshape(mesh.shape["gx"], 4, 4, 4), ALL)
    placed = P("gx", GY)
    return jax.shard_map(
        per_device,
        mesh=torus,
        in_specs=(placed,) * FIELDS,
        out_specs=(placed, placed),
        check_vma=False,
    )
```
